32 devices in a mesh: dp: 16 (over z, y, core), expert: 2 (over x).
Axes of the slice: x: 2, y: 2, z: 4, core: 2. Of those that a mesh axis runs over, the one named last changes fastest.
Arguments:
- tokens: bfloat16 [256, 6144], P(('dp', 'expert')), may hold values from -6 to 6
- router_now: float32 [6144, 8], P('dp'), may hold values from -0.078125 to 0.078125
- router_next: float32 [6144, 8], P('dp'), may hold values from -0.078125 to 0.078125
- w_gate: bfloat16 [8, 6144, 8192], P('expert', None, 'dp'), may hold values from -0.078125 to 0.078125
- w_up: bfloat16 [8, 6144, 8192], P('expert', None, 'dp'), may hold values from -0.078125 to 0.078125
- w_down: bfloat16 [8, 8192, 6144], P('expert', 'dp'), may hold values from -0.0625 to 0.0625
- expert_ids: int32 [256, 2], P(('dp', 'expert')), may hold values from 0 to 7, all different within a row; in each aligned block of 8 rows (0 to 7, 8 to 15, ...) at most 4 rows name the same one
- next_ids: int32 [256, 2], P(('dp', 'expert')), may hold values from 0 to 7, all different within a row
Outputs:
- layer_out: bfloat16 [256, 6144], P(('dp', 'expert'))
- next_logits: float32 [256, 8], P(('dp', 'expert'))
- next_weights: float32 [256, 2], P(('dp', 'expert'))
The draws below stay inside these ranges and needn't reach their ends.
Inputs may be any that keep to these rules, and one draw needn't show every extreme that they name: `expert_ids`: each row names 2 different experts. Among the 8 rows of one device no expert is named by more than 4 rows, and on some devices one expert is named by exactly 4 rows. `next_ids`: each row names 2 different experts.
All inputs are finite; a program needn't handle non-finite values.
Results may differ from the reference program's by a relative error of at most 0.013.
Values may be sent and summed in bfloat16 or wider, within the bound.
A program may use at most 128 MiB of HBM per device.

```python
import math
import jax
import jax.numpy as jnp
import numpy as np
from jax import lax

D = 6144
FF = 8192
EXPERTS = 8
TOP = 2
TOK_DEV = 8
CAP = 4
TOKENS = 256


def levels(rng, extent, shards, low, top_value):
    gain, own = 1.0, jax.random.fold_in(rng, 6)
    for position, parts in shards:
        heights = jnp.exp(jax.random.uniform(jax.random.fold_in(own, position), (parts,), jnp.float32, low / len(shards), top_value / len(shards)))
        gain = gain * jnp.repeat(heights, extent[position] // parts).reshape([-1 if axis == position else 1 for axis in range(len(extent))])
    return gain


def picks_of(rng, rows, amount, top, lift):
    order = jax.random.permutation(jax.random.fold_in(rng, 1), amount)
    favour = order
    for power in range(3):
        favour = favour * favour // amount
    favour = favour * lift // amount
    tickets = jax.random.randint(jax.random.fold_in(rng, 2), (rows, amount), 0, 4096) + favour
    fixed_rows = jax.random.permutation(jax.random.fold_in(rng, 3), rows)[jnp.arange(amount) % rows]
    tickets = jnp.where(jnp.arange(rows)[:, None] == fixed_rows[None, :], 1 << 14, tickets)
    score = tickets * amount + jnp.arange(amount)
    return lax.top_k(score.astype(jnp.int32), top)[1].astype(jnp.int32)


def assign_block(stream_key, own, number, rows, amount, top, limit, slope):
    ranking = jax.random.permutation(stream_key, amount)
    packed, usual = portions_of(amount, rows * top, limit, slope, True), portions_of(amount, rows * top, limit, slope, False)
    places = jnp.arange(amount)

    def named(tallies, turn):
        used = int((tallies > 0).sum())
        fixed = max(1, used // 4)
        moved = fixed + (places - fixed + turn * (used - fixed)) % max(1, amount - fixed)
        return jnp.zeros((amount,), jnp.int32).at[ranking[jnp.where(places < fixed, places, moved)]].set(jnp.asarray(tallies, jnp.int32))

    tallies = jnp.where(number % 4 == 0, named(packed, number // 4), named(usual, number - number // 4 - 1))
    mixed = jax.random.permutation(jax.random.fold_in(own, 3), amount)
    donor, receiver = mixed[0:amount // 2 * 2:2], mixed[1:amount // 2 * 2:2]
    slack = jnp.minimum(tallies[donor] - 1, limit - tallies[receiver]) // 2
    slack = jnp.where((donor == ranking[0]) | (receiver == ranking[0]) | (tallies[receiver] == 0), 0, jnp.maximum(slack, 0))
    moved = jax.random.randint(jax.random.fold_in(own, 4), (amount // 2,), 0, 1 << 20) % (slack + 1)
    tallies = tallies.at[donor].add(-moved).at[receiver].add(moved)
    items = jnp.searchsorted(jnp.cumsum(tallies), jnp.arange(rows * top), side="right").astype(jnp.int32)
    listing = items.reshape(top, rows).T
    listing = listing[jax.random.permutation(jax.random.fold_in(own, 1), rows)]
    turn = jax.random.randint(jax.random.fold_in(own, 2), (rows, 1), 0, top)
    return jnp.take_along_axis(listing, (jnp.arange(top)[None, :] + turn) % top, axis=1)


def portions_of(amount, total, most, skew, full):
    weights = [(1 << 20) // math.isqrt(rank ** skew) + 1 for rank in range(1, amount + 1)]
    largest = most if full else min(most, max(-(-total // amount), total * weights[0] // sum(weights)))
    least = 1 if total - largest >= amount - 1 else 0
    counts, rest = [largest] + [least] * (amount - 1), total - largest - least * (amount - 1)
    while rest > 0:
        candidates = [i for i in range(1, amount) if counts[i] < largest] or [i for i in range(1, amount) if counts[i] < most]
        pool, budget = sum([weights[i] for i in candidates]), rest
        for i in candidates:
            more = min(most - counts[i], max(1, budget * weights[i] // pool), rest)
            counts[i] = counts[i] + more
            rest = rest - more
    return np.array(counts)


def normal_values(own_key, extent, width, most, cuts=(), kind=jnp.bfloat16):
    array = width * jax.random.normal(own_key, extent, jnp.float32)
    if cuts:
        array = array * levels(own_key, extent, cuts, -0.22, 0.18)
    return jnp.clip(array, -most, most).astype(kind)


def setup_inputs(seed: int = 0) -> dict:
    streams_of = jax.random.split(jax.random.key(seed), 9)
    tokens = normal_values(streams_of[0], (TOKENS, D), 1.0, 6.0, ((0, 32),))
    router_now = normal_values(streams_of[1], (D, EXPERTS), D ** -0.5, 0.078125, ((0, 16),), jnp.float32)
    router_next = normal_values(streams_of[2], (D, EXPERTS), D ** -0.5, 0.078125, ((0, 16),), jnp.float32)
    w_gate = normal_values(streams_of[3], (EXPERTS, D, FF), D ** -0.5, 0.078125, ((0, 2), (2, 16)))
    w_up = normal_values(streams_of[4], (EXPERTS, D, FF), D ** -0.5, 0.078125, ((0, 2), (2, 16)))
    w_down = normal_values(streams_of[5], (EXPERTS, FF, D), FF ** -0.5, 0.0625, ((0, 2), (1, 16)))
    expert_ids_keys = jax.random.split(jax.random.fold_in(streams_of[6], 1), TOKENS // TOK_DEV)
    expert_ids_turns = jax.random.permutation(jax.random.fold_in(streams_of[6], 3), TOKENS // TOK_DEV)
    expert_ids = jax.vmap(lambda own, number: assign_block(jax.random.fold_in(streams_of[6], 2), own, number, TOK_DEV, EXPERTS, TOP, CAP, 2))(expert_ids_keys, expert_ids_turns).reshape((TOKENS, TOP))
    next_ids = picks_of(streams_of[7], TOKENS, EXPERTS, TOP, 2048)
    return dict(tokens=tokens, router_now=router_now, router_next=router_next, w_gate=w_gate, w_up=w_up, w_down=w_down, expert_ids=expert_ids, next_ids=next_ids)


epsilon = 1e-05

def rms_normed(values):
    return values * lax.rsqrt(lax.optimization_barrier(jnp.mean(values * values, axis=-1, keepdims=True)) + epsilon)

def pair_weights(logits, chosen):
    picked = jnp.take_along_axis(logits, chosen, axis=1)
    first = jax.nn.sigmoid(picked[:, 0] - picked[:, 1])
    return jnp.stack([first, 1.0 - first], axis=1)

def reference(tokens, router_now, router_next, w_gate, w_up, w_down, expert_ids, next_ids):
    resid = tokens.astype(jnp.float32)
    normed = rms_normed(resid)
    logits = jnp.dot(normed, router_now, precision=lax.Precision.HIGHEST, preferred_element_type=jnp.float32)
    weights = pair_weights(logits, expert_ids)
    rounded = normed.astype(jnp.bfloat16)
    blocks = TOKENS // TOK_DEV
    flat = expert_ids.reshape(blocks, TOK_DEV * TOP)
    onehot = (flat[:, :, None] == jnp.arange(EXPERTS, dtype=jnp.int32)[None, None, :]).astype(jnp.int32)
    ranks = lax.optimization_barrier(jnp.sum((jnp.cumsum(onehot, axis=1) - onehot) * onehot, axis=2)).reshape(TOKENS, TOP).astype(jnp.int32)
    block_of = jnp.broadcast_to((jnp.arange(TOKENS, dtype=jnp.int32) // TOK_DEV)[:, None], (TOKENS, TOP)).astype(jnp.int32)
    buffer = jnp.zeros((blocks, EXPERTS, CAP, D), jnp.bfloat16)
    buffer = buffer.at[block_of, expert_ids, ranks].set(jnp.broadcast_to(rounded[:, None, :], (TOKENS, TOP, D)))
    rows_in = jnp.transpose(buffer, (1, 0, 2, 3)).reshape(EXPERTS, blocks * CAP, D)

    def expert_out(operands):
        inputs, gate_w, up_w, down_w = operands
        gate = jnp.dot(inputs, gate_w, preferred_element_type=jnp.float32)
        upward = jnp.dot(inputs, up_w, preferred_element_type=jnp.float32)
        hidden = (jax.nn.silu(gate) * upward).astype(jnp.bfloat16)
        return jnp.dot(hidden, down_w, preferred_element_type=jnp.float32)
    outputs = lax.map(expert_out, (rows_in, w_gate, w_up, w_down)).reshape(EXPERTS, blocks, CAP, D)
    picked = outputs[expert_ids, block_of, ranks]
    mixture = lax.optimization_barrier(jnp.sum(picked * weights[:, :, None], axis=1))
    summed = resid + mixture
    layer_out = summed.astype(jnp.bfloat16)
    next_logits = jnp.dot(rms_normed(summed), router_next, precision=lax.Precision.HIGHEST, preferred_element_type=jnp.float32)
    next_weights = pair_weights(next_logits, next_ids)
    return (layer_out, next_logits, next_weights)
```

```python
import functools

import jax
import jax.numpy as jnp
from jax import lax
from jax.experimental import pallas as pl
from jax.experimental.pallas import tpu as pltpu
from jax.sharding import PartitionSpec as P

epsilon = 1e-05
BOTH = ("dp", "expert")
ROOM = 1 << 21
CHUNKS = 4
POOL = 28
F32 = jnp.float32
BF16 = jnp.bfloat16


def rms_normed(values):
    return values * lax.rsqrt(jnp.mean(values * values, axis=-1, keepdims=True) + epsilon)


def pair_weights(logits, chosen):
    picked = jnp.take_along_axis(logits, chosen, axis=1)
    first = jax.nn.sigmoid(picked[:, 0] - picked[:, 1])
    return jnp.stack([first, 1.0 - first], axis=1)


def layer_kernel(
    depth,
    tokens_hbm, now_hbm, next_hbm, gate_hbm, up_hbm, down_hbm, ids_ref, next_ids_ref,
    out_ref, logits_ref, weights_ref,
    tok, now_own, now_low, now_all, next_own, next_all, xbuf, pool, acc, hidden,
    part, rd, ra, rb, rz, table,
    local_sem, in_sem, down_sem, small_send, small_recv,
    ag_send, ag_z, ag_pair, ag_core, rs_send, rs_core, rs_first, rs_second, rs_z,
):
    experts, width, units = gate_hbm.shape
    chunks, blocks, per, cols = xbuf.shape
    count = now_own.shape[0]
    mine = now_own.shape[1]
    rows = blocks * per
    groups = width // units
    per_chunk = cols // units
    pieces = chunks * experts * 2
    slots = pool.shape[0] // cols
    late = pieces - slots
    down_base = late * cols
    Z = depth

    d = lax.axis_index("dp")
    x = lax.axis_index("expert")
    core = lax.rem(d, 2)
    y = lax.rem(d // 2, 2)
    z = d // 4

    def peer(dk, dx, dy, dz):
        there = (lax.rem(z + dz, Z) * 2 + lax.rem(y + dy, 2)) * 2 + lax.rem(core + dk, 2)
        return {"dp": there, "expert": lax.rem(x + dx, 2)}

    def remote(src, dst, send, recv, to):
        return pltpu.make_async_remote_copy(
            src_ref=src, dst_ref=dst, send_sem=send, recv_sem=recv,
            device_id=to, device_id_type=pl.DeviceIdType.MESH,
        )

    near = peer(1, 0, 0, 0)

    def in_copy(p, g):
        chunk = p // (2 * experts)
        e = lax.rem(p // 2, experts)
        at = pl.multiple_of(lax.rem(p, slots) * cols, 512)
        source = (gate_hbm, up_hbm)[g].at[e, pl.ds(pl.multiple_of(chunk * cols, 512), cols), :]
        return pltpu.make_async_copy(source, pool.at[pl.ds(at, cols), :], in_sem.at[p])

    def down_copies(n):
        at = pl.ds(pl.multiple_of(n * units, 128), units)
        base = down_base + n * experts * units
        return [
            pltpu.make_async_copy(
                down_hbm.at[e, :, at],
                pool.at[pl.ds(pl.multiple_of(base + e * units, 512), units), :],
                down_sem.at[n, e],
            )
            for e in range(experts)
        ]

    small = [
        pltpu.make_async_copy(tokens_hbm, tok, local_sem.at[0]),
        pltpu.make_async_copy(now_hbm, now_own, local_sem.at[1]),
        pltpu.make_async_copy(next_hbm, next_own, local_sem.at[2]),
    ]
    for copy in small:
        copy.start()

    barrier = pltpu.get_barrier_semaphore()
    others = [
        (dk, dx, dy, dz)
        for dk in range(2) for dx in range(2) for dy in range(2) for dz in range(Z)
    ][1:]
    for to in others:
        pl.semaphore_signal(
            barrier, inc=1, device_id=peer(*to), device_id_type=pl.DeviceIdType.MESH
        )

    def begin(i, carry):
        for g in range(2):
            in_copy(i * 2 + g, g).start()
        return carry

    lax.fori_loop(0, slots // 2, begin, 0)

    small[0].wait()
    resid = tok[...].astype(F32)
    scale = lax.rsqrt(jnp.mean(resid * resid, axis=1, keepdims=True) + epsilon)
    rounded = (resid * scale).astype(BF16)
    for c in range(chunks):
        xbuf[c, 0] = rounded[:, c * cols:(c + 1) * cols]
    small[1].wait()
    own_at = pl.ds(pl.multiple_of(d * mine, 128), mine)
    now_low[...] = now_own[...].astype(BF16)
    now_all[:, own_at] = now_low[...]
    small[2].wait()
    next_all[:, own_at] = next_own[...]

    def clear(i, carry):
        acc[i] = jnp.zeros(acc.shape[1:], F32)
        return carry

    lax.fori_loop(0, acc.shape[0], clear, 0)
    pl.semaphore_wait(barrier, len(others))

    same_side = [to for to in others if to[1] == 0]

    def send_router(own, everyone, i):
        for to in same_side:
            remote(own, everyone.at[:, own_at], small_send.at[i], small_recv.at[i], peer(*to)).start()

    def router_bytes(everyone, i):
        span = everyone.at[:, pl.ds(0, mine * len(same_side))]
        return remote(span, span, small_send.at[i], small_recv.at[i], near)

    def choose(values, ids):
        eye = lax.broadcasted_iota(jnp.int32, (per, per), 0) == lax.broadcasted_iota(
            jnp.int32, (per, per), 1
        )
        names = [
            jnp.sum(jnp.where(eye, ids[i:i + 1, :].astype(F32), 0.0), axis=1, keepdims=True)
            for i in range(2)
        ]
        picked = [
            sum(jnp.where(name == float(e), values[e], 0.0) for e in range(count)) for name in names
        ]
        first = 1.0 / (1.0 + jnp.exp(picked[1] - picked[0]))
        return names, first

    def route():
        router_bytes(now_all, 0).wait_recv()
        whole = now_all[...].astype(F32)
        held = tok[...].astype(F32)
        values = [
            jnp.sum(held * whole[e:e + 1, :], axis=1, keepdims=True) * scale for e in range(count)
        ]
        names, first = choose(values, ids_ref[...])
        lane = lax.broadcasted_iota(jnp.int32, (per, 128), 1).astype(F32)
        table[0] = jnp.where(lane == names[0], first, 0.0) + jnp.where(
            lane == names[1], 1.0 - first, 0.0
        )
        for dk, dx, dy, dz in others:
            slot = ((dk * 2 + dx) * 2 + dy) * Z + (Z - dz) % Z
            remote(
                table.at[0], table.at[slot], small_send.at[1], small_recv.at[1], peer(dk, dx, dy, dz)
            ).start()

    def table_bytes():
        span = table.at[pl.ds(1, len(others))]
        return remote(span, span, small_send.at[1], small_recv.at[1], near)

    own_piece, rest_piece = (0, 1), (1, Z - 1)
    Y_LINE, X_LINE, FAR_LINE, CORE = Z, 2 * Z, 3 * Z, 4 * Z
    y_peer, x_peer = peer(0, 0, 1, 0), peer(0, 1, 0, 0)

    def lines(c):
        return ((Y_LINE, y_peer, X_LINE, x_peer) if c % 2 == 0 else (X_LINE, x_peer, Y_LINE, y_peer))

    def hop(c, which, part_index, source, target, to):
        start, size = (own_piece, rest_piece)[part_index]
        return remote(
            xbuf.at[c, pl.ds(source + start, size)], xbuf.at[c, pl.ds(target + start, size)],
            ag_send.at[c], ag_pair.at[c, which, part_index], to,
        )

    def across(c, i):
        return remote(
            xbuf.at[c, pl.ds(i * Z, Z)], xbuf.at[c, pl.ds(CORE + i * Z, Z)],
            ag_send.at[c], ag_core.at[c, i], near,
        )

    def gather_first(c):
        for dz in range(1, Z):
            remote(
                xbuf.at[c, 0], xbuf.at[c, Z - dz], ag_send.at[c], ag_z.at[c], peer(0, 0, 0, dz)
            ).start()
        a, a_peer, b, b_peer = lines(c)
        hop(c, 0, 0, 0, a, a_peer).start()
        hop(c, 1, 0, 0, b, b_peer).start()

    def gather_own(c):
        a, a_peer, b, b_peer = lines(c)
        hop(c, 0, 0, 0, a, a_peer).wait_recv()
        hop(c, 2, 0, a, FAR_LINE, b_peer).start()

    def gather_line(c):
        span = xbuf.at[c, pl.ds(1, Z - 1)]
        remote(span, span, ag_send.at[c], ag_z.at[c], near).wait_recv()
        a, a_peer, b, b_peer = lines(c)
        hop(c, 0, 1, 0, a, a_peer).start()
        hop(c, 1, 1, 0, b, b_peer).start()
        across(c, 0).start()

    def gather_far(c):
        a, a_peer, b, b_peer = lines(c)
        hop(c, 0, 1, 0, a, a_peer).wait_recv()
        hop(c, 2, 1, a, FAR_LINE, b_peer).start()
        across(c, a // Z).start()

    def gather_second(c):
        a, a_peer, b, b_peer = lines(c)
        for i in range(2):
            hop(c, 1, i, 0, b, b_peer).wait_recv()
        across(c, b // Z).start()

    def gather_last(c):
        a, a_peer, b, b_peer = lines(c)
        for i in range(2):
            hop(c, 2, i, a, FAR_LINE, b_peer).wait_recv()
        across(c, 3).start()

    def gather_done(c):
        for i in range(4):
            across(c, i).wait_recv()

    for c in range(chunks):
        gather_first(c)
    send_router(now_low, now_all, 0)
    for c in range(chunks):
        gather_own(c)
    gather_line(0)
    gather_line(1)
    route()
    gather_far(0)
    gather_line(2)
    gather_far(1)
    gather_second(0)
    gather_line(3)
    gather_last(0)

    hooks = {
        0: [(gather_done, 0), (gather_far, 2), (gather_second, 1)],
        1: [(gather_last, 1), (gather_far, 3)],
        2: [(gather_second, 2)],
        3: [(gather_last, 2)],
        4: [(gather_done, 1), (gather_second, 3)],
        5: [(gather_last, 3)],
        8: [(gather_done, 2)],
        12: [(gather_done, 3)],
    }

    def issue_after(s):
        due = []
        for n in range(groups):
            last = late + -(-((n + 1) * experts * units) // cols) - 1
            if last // 2 == s:
                due.append(n)
        return due

    def ahead(s, carry):
        for step, actions in hooks.items():
            @pl.when(s == step)
            def _(actions=actions):
                for action, c in actions:
                    action(c)

        @pl.when(s == 2 * experts)
        def _():
            send_router(next_own, next_all, 2)

        c = s // experts
        e = lax.rem(s, experts)
        inputs = xbuf[c].reshape(rows, cols)
        for g in range(2):
            p = s * 2 + g
            in_copy(p, g).wait()
            at = pl.multiple_of(lax.rem(p, slots) * cols, 512)
            value = jnp.dot(inputs, pool[pl.ds(at, cols), :], preferred_element_type=F32)
            acc[e * 2 + g] += value

        @pl.when(s < late // 2)
        def _():
            for g in range(2):
                in_copy(slots + s * 2 + g, g).start()

        for step in range(chunks * experts):
            due = issue_after(step)
            if due:
                @pl.when(s == step)
                def _(due=due):
                    for n in due:
                        for copy in down_copies(n):
                            copy.start()

        @pl.when(c == chunks - 1)
        def _():
            @pl.when(e == 0)
            def _():
                table_bytes().wait_recv()

            lane = lax.broadcasted_iota(jnp.int32, (rows, 128), 1)
            shares = table[...].reshape(rows, 128)
            share = jnp.sum(
                jnp.where(lane == x * experts + e, shares, 0.0), axis=1, keepdims=True
            )
            gate = acc[e * 2]
            value = gate / (1.0 + jnp.exp(-gate)) * acc[e * 2 + 1] * share
            hidden[:, pl.ds(pl.multiple_of(e * units, 128), units)] = value.astype(BF16)

        return carry

    lax.fori_loop(0, chunks * experts, ahead, 0)

    def scatter_core(c):
        return remote(
            part.at[c, pl.ds(CORE, CORE)], rd.at[c], rs_send.at[c], rs_core.at[c], near
        )

    def reverse(c):
        return ((X_LINE, x_peer, Y_LINE, y_peer) if c % 2 == 0 else (Y_LINE, y_peer, X_LINE, x_peer))

    def scatter_first(c, i):
        a, a_peer, b, b_peer = reverse(c)
        source = (a, FAR_LINE)[i]
        return remote(
            part.at[c, pl.ds(source, Z)], ra.at[c, i], rs_send.at[c], rs_first.at[c, i], a_peer
        )

    def scatter_second(c):
        a, a_peer, b, b_peer = reverse(c)
        return remote(
            part.at[c, pl.ds(b, Z)], rb.at[c], rs_send.at[c], rs_second.at[c], b_peer
        )

    def add_core(c):
        scatter_core(c).wait_recv()
        a, a_peer, b, b_peer = reverse(c)

        def add(at):
            span = pl.ds(at, Z)
            part[c, span] = (part[c, span].astype(F32) + rd[c, span].astype(F32)).astype(BF16)

        add(FAR_LINE)
        scatter_first(c, 1).start()
        add(a)
        scatter_first(c, 0).start()
        add(b)
        add(0)

    def add_first(c):
        a, a_peer, b, b_peer = reverse(c)
        scatter_first(c, 1).wait_recv()
        span = pl.ds(b, Z)
        part[c, span] = (part[c, span].astype(F32) + ra[c, 1].astype(F32)).astype(BF16)
        scatter_second(c).start()

    def add_second(c):
        scatter_first(c, 0).wait_recv()
        scatter_second(c).wait_recv()
        span = pl.ds(0, Z)
        part[c, span] = (
            part[c, span].astype(F32) + ra[c, 0].astype(F32) + rb[c].astype(F32)
        ).astype(BF16)
        for dz in range(1, Z):
            remote(
                part.at[c, dz], rz.at[c, Z - 1 - dz], rs_send.at[c], rs_z.at[c], peer(0, 0, 0, dz)
            ).start()

    def down(n, carry):
        c = n // per_chunk
        for copy in down_copies(n):
            copy.wait()
        at = pl.multiple_of(down_base + n * experts * units, 512)
        total = jnp.dot(
            hidden[...], pool[pl.ds(at, experts * units), :], preferred_element_type=F32
        )
        lanes = pl.ds(pl.multiple_of(lax.rem(n, per_chunk) * units, 128), units)
        part[c, :, :, lanes] = total.astype(BF16).reshape(blocks, per, units)
        for k in range(chunks):
            @pl.when(n == (k + 1) * per_chunk - 1)
            def _(k=k):
                scatter_core(k).start()
                if k:
                    add_core(k - 1)

        return carry

    lax.fori_loop(0, groups, down, 0)

    router_bytes(next_all, 2).wait_recv()
    held = {"square": jnp.zeros((per, 1), F32), "values": [jnp.zeros((per, 1), F32)] * count}

    def finish(c):
        span = rz.at[c]
        remote(span, span, rs_send.at[c], rs_z.at[c], near).wait_recv()
        at = slice(c * cols, (c + 1) * cols)
        mixture = part[c, 0].astype(F32)
        for i in range(Z - 1):
            mixture = mixture + rz[c, i].astype(F32)
        summed = tok[:, at].astype(F32) + mixture
        out_ref[:, at] = summed.astype(BF16)
        held["square"] = held["square"] + jnp.sum(summed * summed, axis=1, keepdims=True)
        held["values"] = [
            held["values"][e]
            + jnp.sum(summed * next_all[e:e + 1, at], axis=1, keepdims=True)
            for e in range(count)
        ]

    order = [(add_first, 0), (add_core, chunks - 1)]
    for c in range(1, chunks):
        order += [(add_first, c), (add_second, c - 1)]
    order.append((add_second, chunks - 1))
    for action, c in order:
        action(c)
    for c in range(chunks):
        finish(c)

    final = lax.rsqrt(held["square"] / float(width) + epsilon)
    values = [value * final for value in held["values"]]
    place = lax.broadcasted_iota(jnp.int32, (per, count), 1)
    logits_ref[...] = sum(jnp.where(place == e, values[e], 0.0) for e in range(count))
    names, first = choose(values, next_ids_ref[...])
    eye = lax.broadcasted_iota(jnp.int32, (per, per), 0) == lax.broadcasted_iota(
        jnp.int32, (per, per), 1
    )
    for i, value in enumerate((first, 1.0 - first)):
        weights_ref[i:i + 1, :] = jnp.sum(jnp.where(eye, value, 0.0), axis=0, keepdims=True)

    router_bytes(now_all, 0).wait_send()
    router_bytes(next_all, 2).wait_send()
    table_bytes().wait_send()
    for c in range(chunks):
        span = xbuf.at[c, pl.ds(1, blocks - 1)]
        remote(span, span, ag_send.at[c], ag_z.at[c], near).wait_send()
        span = part.at[c, pl.ds(1, blocks - 1)]
        remote(span, span, rs_send.at[c], rs_z.at[c], near).wait_send()


def fused_layer(
    dp, tokens, router_now, router_next, w_gate, w_up, w_down, expert_ids, next_ids
):
    experts, width, units = w_gate.shape
    per = tokens.shape[0]
    mine, count = router_now.shape
    depth = dp // 4
    blocks = dp * 2
    rows = blocks * per
    chunks, cols = CHUNKS, width // CHUNKS
    pieces = chunks * experts * 2
    groups = width // units
    vmem = pl.BlockSpec(memory_space=pltpu.VMEM)
    hbm = pl.BlockSpec(memory_space=pltpu.HBM)
    dma = pltpu.SemaphoreType.DMA
    layer_out, next_logits, next_weights = pl.pallas_call(
        functools.partial(layer_kernel, depth),
        out_shape=[
            jax.ShapeDtypeStruct((per, width), BF16),
            jax.ShapeDtypeStruct((per, count), F32),
            jax.ShapeDtypeStruct((2, per), F32),
        ],
        in_specs=[hbm] * 6 + [vmem] * 2,
        out_specs=[vmem] * 3,
        scratch_shapes=[
            pltpu.VMEM((per, width), BF16),
            pltpu.VMEM((count, mine), F32),
            pltpu.VMEM((count, mine), BF16),
            pltpu.VMEM((count, width), BF16),
            pltpu.VMEM((count, mine), F32),
            pltpu.VMEM((count, width), F32),
            pltpu.VMEM((chunks, blocks, per, cols), BF16),
            pltpu.VMEM((POOL * cols, units), BF16),
            pltpu.VMEM((experts * 2, rows, units), F32),
            pltpu.VMEM((rows, experts * units), BF16),
            pltpu.VMEM((chunks, blocks, per, cols), BF16),
            pltpu.VMEM((chunks, blocks // 2, per, cols), BF16),
            pltpu.VMEM((chunks, 2, depth, per, cols), BF16),
            pltpu.VMEM((chunks, depth, per, cols), BF16),
            pltpu.VMEM((chunks, depth - 1, per, cols), BF16),
            pltpu.VMEM((blocks, per, 128), F32),
            dma((3,)),
            dma((pieces,)),
            dma((groups, experts)),
            dma((3,)),
            dma((3,)),
            dma((chunks,)),
            dma((chunks,)),
            dma((chunks, 3, 2)),
            dma((chunks, 4)),
            dma((chunks,)),
            dma((chunks,)),
            dma((chunks, 2)),
            dma((chunks,)),
            dma((chunks,)),
        ],
        compiler_params=pltpu.CompilerParams(
            vmem_limit_bytes=67043328, collective_id=0, has_side_effects=True
        ),
    )(
        tokens, router_now.T, router_next.T, w_gate, w_up, w_down, expert_ids.T, next_ids.T
    )
    return layer_out, next_logits, next_weights.T


def gathered_layer(tokens, router_now, router_next, w_gate, w_up, w_down, expert_ids, next_ids):
    experts, width, units = w_gate.shape
    count = router_now.shape[1]
    resid = tokens.astype(F32)
    normed = rms_normed(resid)
    pair = lax.all_gather(normed.astype(BF16), "expert", axis=0, tiled=True)
    everyone = lax.all_gather(pair, "dp", axis=0, tiled=True)
    rows = everyone.shape[0]
    routers = jnp.concatenate([router_now.T, router_next.T], axis=0)
    routers = lax.all_gather(routers, "dp", axis=1, tiled=True)
    whole_now, whole_next = routers[:count], routers[count:]
    exact = functools.partial(
        lax.dot_general,
        dimension_numbers=(((1,), (1,)), ((), ())),
        precision=lax.Precision.HIGHEST,
        preferred_element_type=F32,
    )
    logits = exact(normed, whole_now)
    weights = pair_weights(logits, expert_ids)
    named = expert_ids[:, :, None] == jnp.arange(count, dtype=jnp.int32)[None, None, :]
    table = jnp.sum(jnp.where(named, weights[:, :, None], 0.0), axis=1)
    table = lax.all_gather(table, BOTH, axis=0, tiled=True)
    share = lax.dynamic_slice_in_dim(table, lax.axis_index("expert") * experts, experts, axis=1)
    share = share.T[:, :, None]
    total = jnp.zeros((rows, width), F32)
    for e in range(experts):
        gate = jnp.dot(everyone, w_gate[e], preferred_element_type=F32)
        upward = jnp.dot(everyone, w_up[e], preferred_element_type=F32)
        value = gate / (1.0 + jnp.exp(-gate)) * upward * share[e]
        total = total + jnp.dot(value.astype(BF16), w_down[e], preferred_element_type=F32)
    mixture = lax.psum_scatter(total.astype(BF16), "dp", scatter_dimension=0, tiled=True)
    mixture = lax.psum_scatter(mixture, "expert", scatter_dimension=0, tiled=True)
    summed = resid + mixture.astype(F32)
    next_logits = exact(rms_normed(summed), whole_next)
    return (summed.astype(BF16), next_logits, pair_weights(next_logits, next_ids))


def solution(mesh):
    dp, sides = mesh.shape["dp"], mesh.shape["expert"]

    def on_device(tokens, *rest):
        rows, width = tokens.shape[0] * dp * sides, tokens.shape[1]
        if sides == 2 and dp % 4 == 0 and rows * width <= ROOM:
            return fused_layer(dp, tokens, *rest)
        return gathered_layer(tokens, *rest)

    in_specs = (
        P(BOTH, None),
        P("dp", None),
        P("dp", None),
        P("expert", None, "dp"),
        P("expert", None, "dp"),
        P("expert", "dp", None),
        P(BOTH, None),
        P(BOTH, None),
    )
    out_specs = (P(BOTH, None), P(BOTH, None), P(BOTH, None))
    return jax.shard_map(
        on_device, mesh=mesh, in_specs=in_specs, out_specs=out_specs, check_vma=False
    )
```

```python
import functools

import jax
import jax.numpy as jnp
from jax import lax
from jax.experimental import pallas as pl
from jax.experimental.pallas import tpu as pltpu
from jax.sharding import PartitionSpec as P

epsilon = 1e-05
BOTH = ("dp", "expert")
ROOM = 1 << 21
SHARES = (4, 5, 7, 8)
POOL_ROWS = 18432
VMEM_LIMIT = 55000000
PAIR = 2
F32 = jnp.float32
BF16 = jnp.bfloat16


def rms_normed(values):
    return values * lax.rsqrt(jnp.mean(values * values, axis=-1, keepdims=True) + epsilon)


def pair_weights(logits, chosen):
    picked = jnp.take_along_axis(logits, chosen, axis=1)
    first = jax.nn.sigmoid(picked[:, 0] - picked[:, 1])
    return jnp.stack([first, 1.0 - first], axis=1)


def layer_kernel(
    depth, sizes,
    tok, now_own, next_own, gate_hbm, up_hbm, down_hbm, ids_ref, next_ids_ref,
    out_ref, logits_ref, weights_ref,
    now_low, now_all, next_all, xbuf, pool, acc, hidden,
    part, rd, ra, rb, rz, table,
    in_sem, down_sem, small_send, small_recv,
    ag_send, ag_z, ag_pair, ag_core, rs_send, rs_core, rs_first, rs_second, rs_z,
    own_first, own_second,
):
    experts, width, units = gate_hbm.shape
    blocks, per, _ = xbuf.shape
    chunks = len(sizes)
    starts = [sum(sizes[:c]) for c in range(chunks)]
    halves, _, _, _, wide = part.shape
    count = now_own.shape[0]
    mine = now_own.shape[1]
    rows = blocks * per
    groups = width // wide
    space = pool.shape[0]
    deep = experts * units
    Z = depth

    loads, place = [], 0
    for c in range(chunks):
        for e in range(experts):
            loads.append((place, sizes[c]))
            place += sizes[c]
    pieces = len(loads)
    down_base = place % space
    for n in range(groups):
        loads.append((place, deep))
        place += deep
    after = []
    for i, (start, size) in enumerate(loads):
        assert start // space == (start + size - 1) // space
        low, high = start - space, start + size - space
        held = [k for k in range(i) if loads[k][0] < high and sum(loads[k]) > low]
        after.append(max(held, default=-1))
    early = sum(1 for k in after[:pieces] if k < 0)
    assert max(after) < pieces

    d = lax.axis_index("dp")
    x = lax.axis_index("expert")
    core = lax.rem(d, 2)
    y = lax.rem(d // 2, 2)
    z = d // 4

    def peer(dk, dx, dy, dz):
        there = (lax.rem(z + dz, Z) * 2 + lax.rem(y + dy, 2)) * 2 + lax.rem(core + dk, 2)
        return {"dp": there, "expert": lax.rem(x + dx, 2)}

    def remote(src, dst, send, recv, to):
        return pltpu.make_async_remote_copy(
            src_ref=src, dst_ref=dst, send_sem=send, recv_sem=recv,
            device_id=to, device_id_type=pl.DeviceIdType.MESH,
        )

    near = peer(1, 0, 0, 0)

    def in_copies(c, e):
        at = lax.rem(loads[c * experts][0] + e * sizes[c], space)
        at = pl.ds(pl.multiple_of(at, 256), sizes[c])
        rows_at = pl.ds(starts[c], sizes[c])
        return [
            pltpu.make_async_copy(
                w.at[e, rows_at, :], pool.at[at, pl.ds(g * units, units)],
                in_sem.at[c * experts + e, g],
            )
            for g, w in enumerate((gate_hbm, up_hbm))
        ]

    def down_copies(n):
        at = pl.ds(pl.multiple_of(n * wide, 128), wide)
        base = lax.rem(down_base + n * deep, space)
        return [
            pltpu.make_async_copy(
                down_hbm.at[e, :, at],
                pool.at[pl.ds(pl.multiple_of(base + e * units, 512), units), :],
                down_sem.at[n, e],
            )
            for e in range(experts)
        ]

    barrier = pltpu.get_barrier_semaphore()
    others = [
        (dk, dx, dy, dz)
        for dk in range(2) for dx in range(2) for dy in range(2) for dz in range(Z)
    ][1:]
    for to in others:
        pl.semaphore_signal(
            barrier, inc=1, device_id=peer(*to), device_id_type=pl.DeviceIdType.MESH
        )

    for p in range(experts):
        for copy in in_copies(0, p):
            copy.start()

    resid = tok[...].astype(F32)
    scale = lax.rsqrt(jnp.mean(resid * resid, axis=1, keepdims=True) + epsilon)
    rounded = (resid * scale).astype(BF16)
    for c in range(chunks):
        xbuf[0, :, starts[c]:starts[c] + sizes[c]] = rounded[:, starts[c]:starts[c] + sizes[c]]
    own_at = pl.ds(pl.multiple_of(d * mine, 128), mine)
    now_low[...] = now_own[...].astype(BF16)
    pl.semaphore_wait(barrier, len(others))

    same_side = [to for to in others if to[1] == 0]

    def send_router(own, everyone, i):
        for to in same_side:
            remote(own, everyone.at[:, own_at], small_send.at[i], small_recv.at[i], peer(*to)).start()

    def router_bytes(everyone, i):
        span = everyone.at[:, pl.ds(0, mine * len(same_side))]
        return remote(span, span, small_send.at[i], small_recv.at[i], near)

    def choose(values, ids):
        eye = lax.broadcasted_iota(jnp.int32, (per, per), 0) == lax.broadcasted_iota(
            jnp.int32, (per, per), 1
        )
        names = [
            jnp.sum(jnp.where(eye, ids[i:i + 1, :].astype(F32), 0.0), axis=1, keepdims=True)
            for i in range(2)
        ]
        picked = [
            sum(jnp.where(name == float(e), values[e], 0.0) for e in range(count)) for name in names
        ]
        first = 1.0 / (1.0 + jnp.exp(picked[1] - picked[0]))
        return names, first

    def route(c):
        now_all[:, own_at] = now_low[...]
        router_bytes(now_all, 0).wait_recv()
        whole = now_all[...].astype(F32)
        held = tok[...].astype(F32)
        values = [
            jnp.sum(held * whole[e:e + 1, :], axis=1, keepdims=True) * scale for e in range(count)
        ]
        names, first = choose(values, ids_ref[...])
        lane = lax.broadcasted_iota(jnp.int32, (per, 128), 1).astype(F32)
        table[0] = jnp.where(lane == names[0], first, 0.0) + jnp.where(
            lane == names[1], 1.0 - first, 0.0
        )
        for dk, dx, dy, dz in others:
            slot = ((dk * 2 + dx) * 2 + dy) * Z + (Z - dz) % Z
            remote(
                table.at[0], table.at[slot], small_send.at[1], small_recv.at[1], peer(dk, dx, dy, dz)
            ).start()

    def table_bytes():
        span = table.at[pl.ds(1, len(others))]
        return remote(span, span, small_send.at[1], small_recv.at[1], near)

    own_piece, rest_piece = (0, 1), (1, Z - 1)
    Y_LINE, X_LINE, FAR_LINE, CORE = Z, 2 * Z, 3 * Z, 4 * Z
    y_peer, x_peer = peer(0, 0, 1, 0), peer(0, 1, 0, 0)

    def lines(c):
        return ((Y_LINE, y_peer, X_LINE, x_peer) if c % 2 == 0 else (X_LINE, x_peer, Y_LINE, y_peer))

    def piece(c, start, size):
        return xbuf.at[pl.ds(start, size), :, pl.ds(starts[c], sizes[c])]

    def hop(c, which, part_index, source, target, to):
        start, size = (own_piece, rest_piece)[part_index]
        return remote(
            piece(c, source + start, size), piece(c, target + start, size),
            ag_send.at[c], ag_pair.at[c, which, part_index], to,
        )

    def across(c, i):
        return remote(
            piece(c, i * Z, Z), piece(c, CORE + i * Z, Z),
            ag_send.at[c], ag_core.at[c, i], near,
        )

    def gather_first(c):
        a, a_peer, b, b_peer = lines(c)
        hop(c, 0, 0, 0, a, a_peer).start()
        hop(c, 1, 0, 0, b, b_peer).start()
        for dz in range(1, Z):
            remote(
                piece(c, 0, 1), piece(c, Z - dz, 1), ag_send.at[c], ag_z.at[c], peer(0, 0, 0, dz)
            ).start()

    def gather_own(c):
        a, a_peer, b, b_peer = lines(c)
        hop(c, 0, 0, 0, a, a_peer).wait_recv()
        hop(c, 2, 0, a, FAR_LINE, b_peer).start()

    def gather_line(c):
        span = piece(c, 1, Z - 1)
        remote(span, span, ag_send.at[c], ag_z.at[c], near).wait_recv()
        a, a_peer, b, b_peer = lines(c)
        hop(c, 0, 1, 0, a, a_peer).start()
        hop(c, 1, 1, 0, b, b_peer).start()
        across(c, 0).start()

    def gather_far(c):
        a, a_peer, b, b_peer = lines(c)
        hop(c, 0, 1, 0, a, a_peer).wait_recv()
        hop(c, 2, 1, a, FAR_LINE, b_peer).start()
        across(c, a // Z).start()

    def gather_second(c):
        a, a_peer, b, b_peer = lines(c)
        for i in range(2):
            hop(c, 1, i, 0, b, b_peer).wait_recv()
        across(c, b // Z).start()

    def gather_last(c):
        a, a_peer, b, b_peer = lines(c)
        for i in range(2):
            hop(c, 2, i, a, FAR_LINE, b_peer).wait_recv()
        across(c, 3).start()

    def gather_done(c):
        for i in range(4):
            across(c, i).wait_recv()

    for c in range(chunks):
        gather_first(c)
    send_router(now_low, now_all, 0)
    for p in range(experts, early):
        for copy in in_copies(p // experts, p % experts):
            copy.start()

    hooks = {
        -1: [
            (gather_own, 0), (gather_own, 1), (gather_line, 0), (gather_own, 2), (gather_own, 3),
            (gather_line, 1), (gather_far, 0), (gather_second, 0), (gather_line, 2),
            (gather_far, 1), (gather_second, 1), (gather_last, 0), (gather_line, 3),
        ],
        0: [(gather_done, 0)],
        2: [(gather_far, 2), (gather_second, 2), (gather_last, 1)],
        4: [(gather_done, 1), (gather_far, 3)],
        6: [(gather_last, 2), (gather_second, 3), (route, 0)],
        8: [(gather_done, 2)],
        10: [(gather_last, 3)],
        12: [(gather_done, 3)],
    }
    for action, c in hooks.pop(-1):
        action(c)

    freed = {}
    for i in range(early, len(loads)):
        freed.setdefault(max(after[i], 0), []).append(i)

    lane = lax.broadcasted_iota(jnp.int32, (rows, 128), 1)

    def ahead(c, i, carry):
        for step in range(c * experts, (c + 1) * experts, PAIR):
            if step in hooks:
                @pl.when(i * PAIR == step - c * experts)
                def _(actions=hooks[step]):
                    for action, at in actions:
                        action(at)

        for k in range(PAIR):
            for copy in in_copies(c, i * PAIR + k):
                copy.wait()
        for k in range(PAIR):
            e = i * PAIR + k
            at = lax.rem(loads[c * experts][0] + e * sizes[c], space)
            at = pl.ds(pl.multiple_of(at, 256), sizes[c])
            value = jnp.dot(
                xbuf[:, :, starts[c]:starts[c] + sizes[c]].reshape(rows, sizes[c]), pool[at, :],
                preferred_element_type=F32,
            )
            if c == 0:
                acc[e] = value
            elif c < chunks - 1:
                acc[e] += value
            else:
                value = value + acc[e]
                gate, upward = value[:, :units], value[:, units:]
                share = jnp.sum(
                    jnp.where(lane == x * experts + e, table[...].reshape(rows, 128), 0.0),
                    axis=1, keepdims=True,
                )
                value = gate / (1.0 + jnp.exp(-gate)) * upward * share
                hidden[:, pl.ds(pl.multiple_of(e * units, 128), units)] = value.astype(BF16)

        for first in range(c * experts, (c + 1) * experts, PAIR):
            steps = range(first, first + PAIR)
            if any(step in freed for step in steps):
                @pl.when(i * PAIR == first - c * experts)
                def _(steps=steps):
                    for step in steps:
                        for load in freed.get(step, []):
                            if load < pieces:
                                copies = in_copies(load // experts, load % experts)
                            else:
                                copies = down_copies(load - pieces)
                            for copy in copies:
                                copy.start()

        return carry

    for c in range(chunks):
        if c == 1:
            next_all[:, own_at] = next_own[...]
        if c == chunks - 1:
            send_router(next_own, next_all, 2)
            table_bytes().wait_recv()
        lax.fori_loop(0, experts // PAIR, functools.partial(ahead, c), 0)

    REST = pl.ds(1, Z - 1)

    def scatter_core(c):
        h, p = c // 2, c % 2
        return remote(
            part.at[h, p, pl.ds(CORE, CORE)], rd.at[h, p], rs_send.at[0], rs_core.at[h, p], near
        )

    def reverse(p):
        return ((X_LINE, x_peer, Y_LINE, y_peer) if p == 0 else (Y_LINE, y_peer, X_LINE, x_peer))

    def scatter_first(c, i):
        h, p = c // 2, c % 2
        a, a_peer, b, b_peer = reverse(p)
        source = (a, FAR_LINE)[i]
        return remote(
            part.at[h, p, pl.ds(source + 1, Z - 1)], ra.at[h, p, i, REST],
            rs_send.at[0], rs_first.at[h, p, i], a_peer,
        )

    def scatter_second(c):
        h, p = c // 2, c % 2
        a, a_peer, b, b_peer = reverse(p)
        return remote(
            part.at[h, p, pl.ds(b + 1, Z - 1)], rb.at[h, p, REST],
            rs_send.at[0], rs_second.at[h, p], b_peer,
        )

    def layer_first(p, i):
        a, a_peer, b, b_peer = reverse(p)
        source = (a, FAR_LINE)[i]
        return remote(
            part.at[:, p, source], ra.at[:, p, i, 0], rs_send.at[0], own_first.at[p, i], a_peer
        )

    def layer_second(p):
        a, a_peer, b, b_peer = reverse(p)
        return remote(
            part.at[:, p, b], rb.at[:, p, 0], rs_send.at[0], own_second.at[p], b_peer
        )

    def add_core(c):
        h, p = c // 2, c % 2
        scatter_core(c).wait_recv()
        a, a_peer, b, b_peer = reverse(p)

        def add(at):
            span = pl.ds(at, Z)
            part[h, p, span] = (
                part[h, p, span].astype(F32) + rd[h, p, span].astype(F32)
            ).astype(BF16)

        add(FAR_LINE)
        scatter_first(c, 1).start()
        add(a)
        scatter_first(c, 0).start()
        add(b)
        add(0)

    def add_first(c):
        h, p = c // 2, c % 2
        a, a_peer, b, b_peer = reverse(p)
        scatter_first(c, 1).wait_recv()
        span = pl.ds(b + 1, Z - 1)
        part[h, p, span] = (
            part[h, p, span].astype(F32) + ra[h, p, 1, REST].astype(F32)
        ).astype(BF16)
        scatter_second(c).start()

    def add_second(c):
        h, p = c // 2, c % 2
        scatter_first(c, 0).wait_recv()
        scatter_second(c).wait_recv()
        part[h, p, REST] = (
            part[h, p, REST].astype(F32)
            + ra[h, p, 0, REST].astype(F32) + rb[h, p, REST].astype(F32)
        ).astype(BF16)
        for dz in range(1, Z):
            remote(
                part.at[h, p, dz], rz.at[h, p, Z - 1 - dz],
                rs_send.at[0], rs_z.at[h, p], peer(0, 0, 0, dz),
            ).start()

    def layer_send(p):
        for i in (1, 0):
            layer_first(p, i).start()

    def layer_add(p):
        a, a_peer, b, b_peer = reverse(p)
        layer_first(p, 1).wait_recv()
        part[:, p, b] = (part[:, p, b].astype(F32) + ra[:, p, 1, 0].astype(F32)).astype(BF16)
        layer_second(p).start()

    def layer_wait(p):
        layer_first(p, 0).wait_recv()
        layer_second(p).wait_recv()

    ready = {groups - 3: (0,), groups - 2: (1,), groups - 1: (2,)}

    def down(n, carry):
        for copy in down_copies(n):
            copy.wait()
        at = pl.multiple_of(lax.rem(down_base + n * deep, space), 512)
        total = jnp.dot(
            hidden[...], pool[pl.ds(at, experts * units), :], preferred_element_type=F32
        )
        part[n // 2, lax.rem(n, 2)] = total.astype(BF16).reshape(blocks, per, wide)
        for k in range(groups):
            @pl.when(n == k)
            def _(k=k):
                scatter_core(k).start()
                if k:
                    add_core(k - 1)
                for c in ready.get(k, ()):
                    add_first(c)
                if k == groups - 1:
                    add_second(0)

        return carry

    lax.fori_loop(0, groups, down, 0)

    order = [(add_core, groups - 1)]
    for c in range(3, groups):
        if c == groups - 1:
            order += [(layer_send, 0), (layer_send, 1)]
        order += [(add_first, c), (add_second, c - 2)]
    order += [(add_second, groups - 2), (layer_add, 0), (add_second, groups - 1), (layer_add, 1)]
    for action, c in order:
        action(c)
    router_bytes(next_all, 2).wait_recv()

    held = {"square": jnp.zeros((per, 1), F32), "values": [jnp.zeros((per, 1), F32)] * count}

    def finish(c):
        h, p = c // 2, c % 2
        span = rz.at[h, p]
        remote(span, span, rs_send.at[0], rs_z.at[h, p], near).wait_recv()
        at = slice(c * wide, (c + 1) * wide)
        mixture = part[h, p, 0].astype(F32) + ra[h, p, 0, 0].astype(F32) + rb[h, p, 0].astype(F32)
        for i in range(Z - 1):
            mixture = mixture + rz[h, p, i].astype(F32)
        summed = tok[:, at].astype(F32) + mixture
        out_ref[:, at] = summed.astype(BF16)
        held["square"] = held["square"] + jnp.sum(summed * summed, axis=1, keepdims=True)
        held["values"] = [
            held["values"][e]
            + jnp.sum(summed * next_all[e:e + 1, at], axis=1, keepdims=True)
            for e in range(count)
        ]

    for p in range(2):
        layer_wait(p)
    for c in range(groups):
        finish(c)

    final = lax.rsqrt(held["square"] / float(width) + epsilon)
    values = [value * final for value in held["values"]]
    place = lax.broadcasted_iota(jnp.int32, (per, count), 1)
    logits_ref[...] = sum(jnp.where(place == e, values[e], 0.0) for e in range(count))
    names, first = choose(values, next_ids_ref[...])
    eye = lax.broadcasted_iota(jnp.int32, (per, per), 0) == lax.broadcasted_iota(
        jnp.int32, (per, per), 1
    )
    for i, value in enumerate((first, 1.0 - first)):
        weights_ref[i:i + 1, :] = jnp.sum(jnp.where(eye, value, 0.0), axis=0, keepdims=True)

    router_bytes(now_all, 0).wait_send()
    router_bytes(next_all, 2).wait_send()
    table_bytes().wait_send()
    for c in range(chunks):
        span = piece(c, 1, blocks - 1)
        remote(span, span, ag_send.at[c], ag_z.at[c], near).wait_send()
    span = part.at[:, :, pl.ds(1, blocks - 1)]
    remote(span, span, rs_send.at[0], rs_z.at[0, 0], near).wait_send()


def fused_layer(
    dp, tokens, router_now, router_next, w_gate, w_up, w_down, expert_ids, next_ids
):
    experts, width, units = w_gate.shape
    per = tokens.shape[0]
    mine, count = router_now.shape
    depth = dp // 4
    blocks = dp * 2
    rows = blocks * per
    sizes = tuple(width // sum(SHARES) * share for share in SHARES)
    chunks = len(sizes)
    wide = 2 * units
    pieces = chunks * experts
    groups = width // wide
    halves = groups // 2
    vmem = pl.BlockSpec(memory_space=pltpu.VMEM)
    hbm = pl.BlockSpec(memory_space=pltpu.HBM)
    dma = pltpu.SemaphoreType.DMA
    stay = functools.partial(pltpu.with_memory_space_constraint, memory_space=pltpu.HBM)
    layer_out, next_logits, next_weights = pl.pallas_call(
        functools.partial(layer_kernel, depth, sizes),
        out_shape=[
            jax.ShapeDtypeStruct((per, width), BF16),
            jax.ShapeDtypeStruct((per, count), F32),
            jax.ShapeDtypeStruct((2, per), F32),
        ],
        in_specs=[vmem] * 3 + [hbm] * 3 + [vmem] * 2,
        out_specs=[vmem] * 3,
        scratch_shapes=[
            pltpu.VMEM((count, mine), BF16),
            pltpu.VMEM((count, width), BF16),
            pltpu.VMEM((count, width), F32),
            pltpu.VMEM((blocks, per, width), BF16),
            pltpu.VMEM((POOL_ROWS, wide), BF16),
            pltpu.VMEM((experts, rows, wide), F32),
            pltpu.VMEM((rows, experts * units), BF16),
            pltpu.VMEM((halves, 2, blocks, per, wide), BF16),
            pltpu.VMEM((halves, 2, blocks // 2, per, wide), BF16),
            pltpu.VMEM((halves, 2, 2, depth, per, wide), BF16),
            pltpu.VMEM((halves, 2, depth, per, wide), BF16),
            pltpu.VMEM((halves, 2, depth - 1, per, wide), BF16),
            pltpu.VMEM((blocks, per, 128), F32),
            dma((pieces, 2)),
            dma((groups, experts)),
            dma((3,)),
            dma((3,)),
            dma((chunks,)),
            dma((chunks,)),
            dma((chunks, 3, 2)),
            dma((chunks, 4)),
            dma((1,)),
            dma((halves, 2)),
            dma((halves, 2, 2)),
            dma((halves, 2)),
            dma((halves, 2)),
            dma((2, 2)),
            dma((2,)),
        ],
        compiler_params=pltpu.CompilerParams(
            vmem_limit_bytes=VMEM_LIMIT, collective_id=0, has_side_effects=True
        ),
    )(
        *[stay(value) for value in (tokens, router_now.T, router_next.T)],
        w_gate, w_up, w_down, stay(expert_ids.T), stay(next_ids.T),
    )
    return layer_out, next_logits, next_weights.T


def gathered_layer(tokens, router_now, router_next, w_gate, w_up, w_down, expert_ids, next_ids):
    experts, width, units = w_gate.shape
    count = router_now.shape[1]
    resid = tokens.astype(F32)
    normed = rms_normed(resid)
    pair = lax.all_gather(normed.astype(BF16), "expert", axis=0, tiled=True)
    everyone = lax.all_gather(pair, "dp", axis=0, tiled=True)
    rows = everyone.shape[0]
    routers = jnp.concatenate([router_now.T, router_next.T], axis=0)
    routers = lax.all_gather(routers, "dp", axis=1, tiled=True)
    whole_now, whole_next = routers[:count], routers[count:]
    exact = functools.partial(
        lax.dot_general,
        dimension_numbers=(((1,), (1,)), ((), ())),
        precision=lax.Precision.HIGHEST,
        preferred_element_type=F32,
    )
    logits = exact(normed, whole_now)
    weights = pair_weights(logits, expert_ids)
    named = expert_ids[:, :, None] == jnp.arange(count, dtype=jnp.int32)[None, None, :]
    table = jnp.sum(jnp.where(named, weights[:, :, None], 0.0), axis=1)
    table = lax.all_gather(table, BOTH, axis=0, tiled=True)
    share = lax.dynamic_slice_in_dim(table, lax.axis_index("expert") * experts, experts, axis=1)
    share = share.T[:, :, None]
    total = jnp.zeros((rows, width), F32)
    for e in range(experts):
        gate = jnp.dot(everyone, w_gate[e], preferred_element_type=F32)
        upward = jnp.dot(everyone, w_up[e], preferred_element_type=F32)
        value = gate / (1.0 + jnp.exp(-gate)) * upward * share[e]
        total = total + jnp.dot(value.astype(BF16), w_down[e], preferred_element_type=F32)
    mixture = lax.psum_scatter(total.astype(BF16), "dp", scatter_dimension=0, tiled=True)
    mixture = lax.psum_scatter(mixture, "expert", scatter_dimension=0, tiled=True)
    summed = resid + mixture.astype(F32)
    next_logits = exact(rms_normed(summed), whole_next)
    return (summed.astype(BF16), next_logits, pair_weights(next_logits, next_ids))


def solution(mesh):
    dp, sides = mesh.shape["dp"], mesh.shape["expert"]

    def on_device(tokens, *rest):
        rows, width = tokens.shape[0] * dp * sides, tokens.shape[1]
        if sides == 2 and dp % 4 == 0 and rows * width <= ROOM:
            return fused_layer(dp, tokens, *rest)
        return gathered_layer(tokens, *rest)

    in_specs = (
        P(BOTH, None),
        P("dp", None),
        P("dp", None),
        P("expert", None, "dp"),
        P("expert", None, "dp"),
        P("expert", "dp", None),
        P(BOTH, None),
        P(BOTH, None),
    )
    out_specs = (P(BOTH, None), P(BOTH, None), P(BOTH, None))
    return jax.shard_map(
        on_device, mesh=mesh, in_specs=in_specs, out_specs=out_specs, check_vma=False
    )
```

```python
import functools

import jax
import jax.numpy as jnp
from jax import lax
from jax.experimental import pallas as pl
from jax.experimental.pallas import tpu as pltpu
from jax.sharding import PartitionSpec as P

epsilon = 1e-05
BOTH = ("dp", "expert")
ROOM = 1 << 21
SHARES = (4, 5, 7, 8)
POOL_ROWS = 18432
VMEM_LIMIT = 55000000
PAIR = 2
F32 = jnp.float32
BF16 = jnp.bfloat16


def rms_normed(values):
    return values * lax.rsqrt(jnp.mean(values * values, axis=-1, keepdims=True) + epsilon)


def pair_weights(logits, chosen):
    picked = jnp.take_along_axis(logits, chosen, axis=1)
    first = jax.nn.sigmoid(picked[:, 0] - picked[:, 1])
    return jnp.stack([first, 1.0 - first], axis=1)


def layer_kernel(
    depth, sizes,
    tokens_hbm, now_hbm, next_hbm, gate_hbm, up_hbm, down_hbm, ids_hbm, next_ids_hbm,
    out_ref, logits_ref, weights_ref,
    tok, now_own, next_own, ids_ref, next_ids_ref, now_low, now_all, next_all, xbuf, pool, acc, hidden,
    part, rd, ra, rb, rz, table,
    local_sem, in_sem, down_sem, small_send, small_recv,
    ag_send, ag_z, ag_pair, ag_core, rs_send, rs_core, rs_first, rs_second, rs_z,
    own_first, own_second,
):
    experts, width, units = gate_hbm.shape
    blocks, per, _ = xbuf.shape
    chunks = len(sizes)
    starts = [sum(sizes[:c]) for c in range(chunks)]
    halves, _, _, _, wide = part.shape
    count = now_own.shape[0]
    mine = now_own.shape[1]
    rows = blocks * per
    groups = width // wide
    space = pool.shape[0]
    deep = experts * units
    Z = depth

    loads, place = [], 0
    for c in range(chunks):
        for e in range(experts):
            loads.append((place, sizes[c]))
            place += sizes[c]
    pieces = len(loads)
    down_base = place % space
    for n in range(groups):
        loads.append((place, deep))
        place += deep
    after = []
    for i, (start, size) in enumerate(loads):
        assert start // space == (start + size - 1) // space
        low, high = start - space, start + size - space
        held = [k for k in range(i) if loads[k][0] < high and sum(loads[k]) > low]
        after.append(max(held, default=-1))
    early = sum(1 for k in after[:pieces] if k < 0)
    assert max(after) < pieces

    d = lax.axis_index("dp")
    x = lax.axis_index("expert")
    core = lax.rem(d, 2)
    y = lax.rem(d // 2, 2)
    z = d // 4

    def peer(dk, dx, dy, dz):
        there = (lax.rem(z + dz, Z) * 2 + lax.rem(y + dy, 2)) * 2 + lax.rem(core + dk, 2)
        return {"dp": there, "expert": lax.rem(x + dx, 2)}

    def remote(src, dst, send, recv, to):
        return pltpu.make_async_remote_copy(
            src_ref=src, dst_ref=dst, send_sem=send, recv_sem=recv,
            device_id=to, device_id_type=pl.DeviceIdType.MESH,
        )

    near = peer(1, 0, 0, 0)

    def in_copies(c, e):
        at = lax.rem(loads[c * experts][0] + e * sizes[c], space)
        at = pl.ds(pl.multiple_of(at, 256), sizes[c])
        rows_at = pl.ds(starts[c], sizes[c])
        return [
            pltpu.make_async_copy(
                w.at[e, rows_at, :], pool.at[at, pl.ds(g * units, units)],
                in_sem.at[c * experts + e, g],
            )
            for g, w in enumerate((gate_hbm, up_hbm))
        ]

    def down_copies(n):
        at = pl.ds(pl.multiple_of(n * wide, 128), wide)
        base = lax.rem(down_base + n * deep, space)
        return [
            pltpu.make_async_copy(
                down_hbm.at[e, :, at],
                pool.at[pl.ds(pl.multiple_of(base + e * units, 512), units), :],
                down_sem.at[n, e],
            )
            for e in range(experts)
        ]

    small = [
        pltpu.make_async_copy(source, target, local_sem.at[i])
        for i, (source, target) in enumerate((
            (tokens_hbm, tok), (now_hbm, now_own), (next_hbm, next_own),
            (ids_hbm, ids_ref), (next_ids_hbm, next_ids_ref),
        ))
    ]
    small[0].start()
    barrier = pltpu.get_barrier_semaphore()
    others = [
        (dk, dx, dy, dz)
        for dk in range(2) for dx in range(2) for dy in range(2) for dz in range(Z)
    ][1:]
    for to in others:
        pl.semaphore_signal(
            barrier, inc=1, device_id=peer(*to), device_id_type=pl.DeviceIdType.MESH
        )

    for copy in small[1:]:
        copy.start()
    for p in range(experts):
        for copy in in_copies(0, p):
            copy.start()

    small[0].wait()
    resid = tok[...].astype(F32)
    scale = lax.rsqrt(jnp.mean(resid * resid, axis=1, keepdims=True) + epsilon)
    rounded = (resid * scale).astype(BF16)
    for c in range(chunks):
        xbuf[0, :, starts[c]:starts[c] + sizes[c]] = rounded[:, starts[c]:starts[c] + sizes[c]]
    own_at = pl.ds(pl.multiple_of(d * mine, 128), mine)
    pl.semaphore_wait(barrier, len(others))

    same_side = [to for to in others if to[1] == 0]

    def send_router(own, everyone, i):
        for to in same_side:
            remote(own, everyone.at[:, own_at], small_send.at[i], small_recv.at[i], peer(*to)).start()

    def router_bytes(everyone, i):
        span = everyone.at[:, pl.ds(0, mine * len(same_side))]
        return remote(span, span, small_send.at[i], small_recv.at[i], near)

    def choose(values, ids):
        eye = lax.broadcasted_iota(jnp.int32, (per, per), 0) == lax.broadcasted_iota(
            jnp.int32, (per, per), 1
        )
        names = [
            jnp.sum(jnp.where(eye, ids[i:i + 1, :].astype(F32), 0.0), axis=1, keepdims=True)
            for i in range(2)
        ]
        picked = [
            sum(jnp.where(name == float(e), values[e], 0.0) for e in range(count)) for name in names
        ]
        first = 1.0 / (1.0 + jnp.exp(picked[1] - picked[0]))
        return names, first

    def route(c):
        now_all[:, own_at] = now_low[...]
        router_bytes(now_all, 0).wait_recv()
        whole = now_all[...].astype(F32)
        held = tok[...].astype(F32)
        values = [
            jnp.sum(held * whole[e:e + 1, :], axis=1, keepdims=True) * scale for e in range(count)
        ]
        names, first = choose(values, ids_ref[...])
        lane = lax.broadcasted_iota(jnp.int32, (per, 128), 1).astype(F32)
        table[0] = jnp.where(lane == names[0], first, 0.0) + jnp.where(
            lane == names[1], 1.0 - first, 0.0
        )
        for dk, dx, dy, dz in others:
            slot = ((dk * 2 + dx) * 2 + dy) * Z + (Z - dz) % Z
            remote(
                table.at[0], table.at[slot], small_send.at[1], small_recv.at[1], peer(dk, dx, dy, dz)
            ).start()

    def table_bytes():
        span = table.at[pl.ds(1, len(others))]
        return remote(span, span, small_send.at[1], small_recv.at[1], near)

    own_piece, rest_piece = (0, 1), (1, Z - 1)
    Y_LINE, X_LINE, FAR_LINE, CORE = Z, 2 * Z, 3 * Z, 4 * Z
    y_peer, x_peer = peer(0, 0, 1, 0), peer(0, 1, 0, 0)

    def lines(c):
        return ((Y_LINE, y_peer, X_LINE, x_peer) if c % 2 == 0 else (X_LINE, x_peer, Y_LINE, y_peer))

    def piece(c, start, size):
        return xbuf.at[pl.ds(start, size), :, pl.ds(starts[c], sizes[c])]

    def hop(c, which, part_index, source, target, to):
        start, size = (own_piece, rest_piece)[part_index]
        return remote(
            piece(c, source + start, size), piece(c, target + start, size),
            ag_send.at[c], ag_pair.at[c, which, part_index], to,
        )

    def across(c, i):
        return remote(
            piece(c, i * Z, Z), piece(c, CORE + i * Z, Z),
            ag_send.at[c], ag_core.at[c, i], near,
        )

    def gather_first(c):
        a, a_peer, b, b_peer = lines(c)
        hop(c, 0, 0, 0, a, a_peer).start()
        hop(c, 1, 0, 0, b, b_peer).start()
        for dz in range(1, Z):
            remote(
                piece(c, 0, 1), piece(c, Z - dz, 1), ag_send.at[c], ag_z.at[c], peer(0, 0, 0, dz)
            ).start()

    def gather_own(c):
        a, a_peer, b, b_peer = lines(c)
        hop(c, 0, 0, 0, a, a_peer).wait_recv()
        hop(c, 2, 0, a, FAR_LINE, b_peer).start()

    def gather_line(c):
        span = piece(c, 1, Z - 1)
        remote(span, span, ag_send.at[c], ag_z.at[c], near).wait_recv()
        a, a_peer, b, b_peer = lines(c)
        hop(c, 0, 1, 0, a, a_peer).start()
        hop(c, 1, 1, 0, b, b_peer).start()
        across(c, 0).start()

    def gather_far(c):
        a, a_peer, b, b_peer = lines(c)
        hop(c, 0, 1, 0, a, a_peer).wait_recv()
        hop(c, 2, 1, a, FAR_LINE, b_peer).start()
        across(c, a // Z).start()

    def gather_second(c):
        a, a_peer, b, b_peer = lines(c)
        for i in range(2):
            hop(c, 1, i, 0, b, b_peer).wait_recv()
        across(c, b // Z).start()

    def gather_last(c):
        a, a_peer, b, b_peer = lines(c)
        for i in range(2):
            hop(c, 2, i, a, FAR_LINE, b_peer).wait_recv()
        across(c, 3).start()

    def gather_done(c):
        for i in range(4):
            across(c, i).wait_recv()

    for c in range(chunks):
        gather_first(c)
    for copy in small[1:]:
        copy.wait()
    now_low[...] = now_own[...].astype(BF16)
    send_router(now_low, now_all, 0)
    for p in range(experts, early):
        for copy in in_copies(p // experts, p % experts):
            copy.start()

    hooks = {
        -1: [
            (gather_own, 0), (gather_own, 1), (gather_line, 0), (gather_own, 2), (gather_own, 3),
            (gather_line, 1), (gather_far, 0), (gather_second, 0), (gather_far, 1),
            (gather_second, 1), (gather_line, 2), (gather_last, 0), (gather_line, 3),
        ],
        0: [(gather_done, 0)],
        2: [(gather_last, 1)],
        4: [(gather_far, 2), (gather_second, 2), (gather_done, 1)],
        6: [(route, 0), (gather_far, 3)],
        8: [(gather_last, 2), (gather_second, 3), (gather_done, 2)],
        10: [(gather_last, 3)],
        12: [(gather_done, 3)],
    }
    for action, c in hooks.pop(-1):
        action(c)

    freed = {}
    for i in range(early, len(loads)):
        freed.setdefault(max(after[i], 0), []).append(i)

    lane = lax.broadcasted_iota(jnp.int32, (rows, 128), 1)

    def ahead(c, i, carry):
        for step in range(c * experts, (c + 1) * experts, PAIR):
            if step in hooks:
                @pl.when(i * PAIR == step - c * experts)
                def _(actions=hooks[step]):
                    for action, at in actions:
                        action(at)

        for k in range(PAIR):
            for copy in in_copies(c, i * PAIR + k):
                copy.wait()
        for k in range(PAIR):
            e = i * PAIR + k
            at = lax.rem(loads[c * experts][0] + e * sizes[c], space)
            at = pl.ds(pl.multiple_of(at, 256), sizes[c])
            value = jnp.dot(
                xbuf[:, :, starts[c]:starts[c] + sizes[c]].reshape(rows, sizes[c]), pool[at, :],
                preferred_element_type=F32,
            )
            if c == 0:
                acc[e] = value
            elif c < chunks - 1:
                acc[e] += value
            else:
                value = value + acc[e]
                gate, upward = value[:, :units], value[:, units:]
                share = jnp.sum(
                    jnp.where(lane == x * experts + e, table[...].reshape(rows, 128), 0.0),
                    axis=1, keepdims=True,
                )
                value = gate / (1.0 + jnp.exp(-gate)) * upward * share
                hidden[:, pl.ds(pl.multiple_of(e * units, 128), units)] = value.astype(BF16)

        for first in range(c * experts, (c + 1) * experts, PAIR):
            steps = range(first, first + PAIR)
            if any(step in freed for step in steps):
                @pl.when(i * PAIR == first - c * experts)
                def _(steps=steps):
                    for step in steps:
                        for load in freed.get(step, []):
                            if load < pieces:
                                copies = in_copies(load // experts, load % experts)
                            else:
                                copies = down_copies(load - pieces)
                            for copy in copies:
                                copy.start()

        return carry

    for c in range(chunks):
        if c == 1:
            next_all[:, own_at] = next_own[...]
        if c == chunks - 1:
            send_router(next_own, next_all, 2)
            table_bytes().wait_recv()
        lax.fori_loop(0, experts // PAIR, functools.partial(ahead, c), 0)

    REST = pl.ds(1, Z - 1)

    def scatter_core(c):
        h, p = c // 2, c % 2
        return remote(
            part.at[h, p, pl.ds(CORE, CORE)], rd.at[h, p], rs_send.at[0], rs_core.at[h, p], near
        )

    def reverse(p):
        return ((X_LINE, x_peer, Y_LINE, y_peer) if p == 0 else (Y_LINE, y_peer, X_LINE, x_peer))

    def scatter_first(c, i):
        h, p = c // 2, c % 2
        a, a_peer, b, b_peer = reverse(p)
        source = (a, FAR_LINE)[i]
        return remote(
            part.at[h, p, pl.ds(source + 1, Z - 1)], ra.at[h, p, i, REST],
            rs_send.at[0], rs_first.at[h, p, i], a_peer,
        )

    def scatter_second(c):
        h, p = c // 2, c % 2
        a, a_peer, b, b_peer = reverse(p)
        return remote(
            part.at[h, p, pl.ds(b + 1, Z - 1)], rb.at[h, p, REST],
            rs_send.at[0], rs_second.at[h, p], b_peer,
        )

    def layer_first(p, i):
        a, a_peer, b, b_peer = reverse(p)
        source = (a, FAR_LINE)[i]
        return remote(
            part.at[:, p, source], ra.at[:, p, i, 0], rs_send.at[0], own_first.at[p, i], a_peer
        )

    def layer_second(p):
        a, a_peer, b, b_peer = reverse(p)
        return remote(
            part.at[:, p, b], rb.at[:, p, 0], rs_send.at[0], own_second.at[p], b_peer
        )

    def add_core(c):
        h, p = c // 2, c % 2
        scatter_core(c).wait_recv()
        a, a_peer, b, b_peer = reverse(p)

        def add(at):
            span = pl.ds(at, Z)
            part[h, p, span] = (
                part[h, p, span].astype(F32) + rd[h, p, span].astype(F32)
            ).astype(BF16)

        add(FAR_LINE)
        scatter_first(c, 1).start()
        add(a)
        scatter_first(c, 0).start()
        add(b)
        add(0)

    def add_first(c):
        h, p = c // 2, c % 2
        a, a_peer, b, b_peer = reverse(p)
        scatter_first(c, 1).wait_recv()
        span = pl.ds(b + 1, Z - 1)
        part[h, p, span] = (
            part[h, p, span].astype(F32) + ra[h, p, 1, REST].astype(F32)
        ).astype(BF16)
        scatter_second(c).start()

    def add_second(c):
        h, p = c // 2, c % 2
        scatter_first(c, 0).wait_recv()
        scatter_second(c).wait_recv()
        part[h, p, REST] = (
            part[h, p, REST].astype(F32)
            + ra[h, p, 0, REST].astype(F32) + rb[h, p, REST].astype(F32)
        ).astype(BF16)
        for dz in range(1, Z):
            remote(
                part.at[h, p, dz], rz.at[h, p, Z - 1 - dz],
                rs_send.at[0], rs_z.at[h, p], peer(0, 0, 0, dz),
            ).start()

    def layer_send(p):
        for i in (1, 0):
            layer_first(p, i).start()

    def layer_add(p):
        a, a_peer, b, b_peer = reverse(p)
        layer_first(p, 1).wait_recv()
        part[:, p, b] = (part[:, p, b].astype(F32) + ra[:, p, 1, 0].astype(F32)).astype(BF16)
        layer_second(p).start()

    def layer_wait(p):
        layer_first(p, 0).wait_recv()
        layer_second(p).wait_recv()

    ready = {groups - 3: (0,), groups - 2: (1,), groups - 1: (2,)}

    def down(n, carry):
        for copy in down_copies(n):
            copy.wait()
        at = pl.multiple_of(lax.rem(down_base + n * deep, space), 512)
        total = jnp.dot(
            hidden[...], pool[pl.ds(at, experts * units), :], preferred_element_type=F32
        )
        part[n // 2, lax.rem(n, 2)] = total.astype(BF16).reshape(blocks, per, wide)
        for k in range(groups):
            @pl.when(n == k)
            def _(k=k):
                scatter_core(k).start()
                if k:
                    add_core(k - 1)
                for c in ready.get(k, ()):
                    add_first(c)
                if k == groups - 1:
                    add_second(0)

        return carry

    lax.fori_loop(0, groups, down, 0)

    held = {"square": jnp.zeros((per, 1), F32), "values": [jnp.zeros((per, 1), F32)] * count}

    def finish(c):
        h, p = c // 2, c % 2
        span = rz.at[h, p]
        remote(span, span, rs_send.at[0], rs_z.at[h, p], near).wait_recv()
        at = slice(c * wide, (c + 1) * wide)
        mixture = part[h, p, 0].astype(F32) + ra[h, p, 0, 0].astype(F32) + rb[h, p, 0].astype(F32)
        for i in range(Z - 1):
            mixture = mixture + rz[h, p, i].astype(F32)
        summed = tok[:, at].astype(F32) + mixture
        out_ref[:, at] = summed.astype(BF16)
        held["square"] = held["square"] + jnp.sum(summed * summed, axis=1, keepdims=True)
        held["values"] = [
            held["values"][e]
            + jnp.sum(summed * next_all[e:e + 1, at], axis=1, keepdims=True)
            for e in range(count)
        ]

    def next_wait(i):
        router_bytes(next_all, i).wait_recv()

    last = groups - 1
    order = [(add_core, last)]
    for c in range(3, groups):
        order += [(add_first, c), (add_second, c - 2)]
    order[-1:-1] = [(layer_send, 0), (layer_send, 1)]
    order += [(add_second, last - 1), (add_second, last), (layer_add, 0), (layer_add, 1)]
    order += [(next_wait, 2), (layer_wait, 0)] + [(finish, c) for c in range(0, last - 1, 2)]
    order += [(layer_wait, 1)] + [(finish, c) for c in range(1, last, 2)]
    order += [(finish, last - 1), (finish, last)]
    for action, c in order:
        action(c)

    final = lax.rsqrt(held["square"] / float(width) + epsilon)
    values = [value * final for value in held["values"]]
    place = lax.broadcasted_iota(jnp.int32, (per, count), 1)
    logits_ref[...] = sum(jnp.where(place == e, values[e], 0.0) for e in range(count))
    names, first = choose(values, next_ids_ref[...])
    eye = lax.broadcasted_iota(jnp.int32, (per, per), 0) == lax.broadcasted_iota(
        jnp.int32, (per, per), 1
    )
    for i, value in enumerate((first, 1.0 - first)):
        weights_ref[i:i + 1, :] = jnp.sum(jnp.where(eye, value, 0.0), axis=0, keepdims=True)

    router_bytes(now_all, 0).wait_send()
    router_bytes(next_all, 2).wait_send()
    table_bytes().wait_send()
    for c in range(chunks):
        span = piece(c, 1, blocks - 1)
        remote(span, span, ag_send.at[c], ag_z.at[c], near).wait_send()
    span = part.at[:, :, pl.ds(1, blocks - 1)]
    remote(span, span, rs_send.at[0], rs_z.at[0, 0], near).wait_send()


def fused_layer(
    dp, tokens, router_now, router_next, w_gate, w_up, w_down, expert_ids, next_ids
):
    experts, width, units = w_gate.shape
    per = tokens.shape[0]
    mine, count = router_now.shape
    depth = dp // 4
    blocks = dp * 2
    rows = blocks * per
    sizes = tuple(width // sum(SHARES) * share for share in SHARES)
    chunks = len(sizes)
    wide = 2 * units
    pieces = chunks * experts
    groups = width // wide
    halves = groups // 2
    vmem = pl.BlockSpec(memory_space=pltpu.VMEM)
    hbm = pl.BlockSpec(memory_space=pltpu.HBM)
    dma = pltpu.SemaphoreType.DMA
    stay = functools.partial(pltpu.with_memory_space_constraint, memory_space=pltpu.HBM)
    layer_out, next_logits, next_weights = pl.pallas_call(
        functools.partial(layer_kernel, depth, sizes),
        out_shape=[
            jax.ShapeDtypeStruct((per, width), BF16),
            jax.ShapeDtypeStruct((per, count), F32),
            jax.ShapeDtypeStruct((2, per), F32),
        ],
        in_specs=[hbm] * 8,
        out_specs=[vmem] * 3,
        scratch_shapes=[
            pltpu.VMEM((per, width), BF16),
            pltpu.VMEM((count, mine), F32),
            pltpu.VMEM((count, mine), F32),
            pltpu.VMEM((2, per), jnp.int32),
            pltpu.VMEM((2, per), jnp.int32),
            pltpu.VMEM((count, mine), BF16),
            pltpu.VMEM((count, width), BF16),
            pltpu.VMEM((count, width), F32),
            pltpu.VMEM((blocks, per, width), BF16),
            pltpu.VMEM((POOL_ROWS, wide), BF16),
            pltpu.VMEM((experts, rows, wide), F32),
            pltpu.VMEM((rows, experts * units), BF16),
            pltpu.VMEM((halves, 2, blocks, per, wide), BF16),
            pltpu.VMEM((halves, 2, blocks // 2, per, wide), BF16),
            pltpu.VMEM((halves, 2, 2, depth, per, wide), BF16),
            pltpu.VMEM((halves, 2, depth, per, wide), BF16),
            pltpu.VMEM((halves, 2, depth - 1, per, wide), BF16),
            pltpu.VMEM((blocks, per, 128), F32),
            dma((5,)),
            dma((pieces, 2)),
            dma((groups, experts)),
            dma((3,)),
            dma((3,)),
            dma((chunks,)),
            dma((chunks,)),
            dma((chunks, 3, 2)),
            dma((chunks, 4)),
            dma((1,)),
            dma((halves, 2)),
            dma((halves, 2, 2)),
            dma((halves, 2)),
            dma((halves, 2)),
            dma((2, 2)),
            dma((2,)),
        ],
        compiler_params=pltpu.CompilerParams(
            vmem_limit_bytes=VMEM_LIMIT, collective_id=0, has_side_effects=True
        ),
    )(
        *[stay(value) for value in (tokens, router_now.T, router_next.T)],
        w_gate, w_up, w_down, stay(expert_ids.T), stay(next_ids.T),
    )
    return layer_out, next_logits, next_weights.T


def gathered_layer(tokens, router_now, router_next, w_gate, w_up, w_down, expert_ids, next_ids):
    experts, width, units = w_gate.shape
    count = router_now.shape[1]
    resid = tokens.astype(F32)
    normed = rms_normed(resid)
    pair = lax.all_gather(normed.astype(BF16), "expert", axis=0, tiled=True)
    everyone = lax.all_gather(pair, "dp", axis=0, tiled=True)
    rows = everyone.shape[0]
    routers = jnp.concatenate([router_now.T, router_next.T], axis=0)
    routers = lax.all_gather(routers, "dp", axis=1, tiled=True)
    whole_now, whole_next = routers[:count], routers[count:]
    exact = functools.partial(
        lax.dot_general,
        dimension_numbers=(((1,), (1,)), ((), ())),
        precision=lax.Precision.HIGHEST,
        preferred_element_type=F32,
    )
    logits = exact(normed, whole_now)
    weights = pair_weights(logits, expert_ids)
    named = expert_ids[:, :, None] == jnp.arange(count, dtype=jnp.int32)[None, None, :]
    table = jnp.sum(jnp.where(named, weights[:, :, None], 0.0), axis=1)
    table = lax.all_gather(table, BOTH, axis=0, tiled=True)
    share = lax.dynamic_slice_in_dim(table, lax.axis_index("expert") * experts, experts, axis=1)
    share = share.T[:, :, None]
    total = jnp.zeros((rows, width), F32)
    for e in range(experts):
        gate = jnp.dot(everyone, w_gate[e], preferred_element_type=F32)
        upward = jnp.dot(everyone, w_up[e], preferred_element_type=F32)
        value = gate / (1.0 + jnp.exp(-gate)) * upward * share[e]
        total = total + jnp.dot(value.astype(BF16), w_down[e], preferred_element_type=F32)
    mixture = lax.psum_scatter(total.astype(BF16), "dp", scatter_dimension=0, tiled=True)
    mixture = lax.psum_scatter(mixture, "expert", scatter_dimension=0, tiled=True)
    summed = resid + mixture.astype(F32)
    next_logits = exact(rms_normed(summed), whole_next)
    return (summed.astype(BF16), next_logits, pair_weights(next_logits, next_ids))


def solution(mesh):
    dp, sides = mesh.shape["dp"], mesh.shape["expert"]

    def on_device(tokens, *rest):
        rows, width = tokens.shape[0] * dp * sides, tokens.shape[1]
        if sides == 2 and dp % 4 == 0 and rows * width <= ROOM:
            return fused_layer(dp, tokens, *rest)
        return gathered_layer(tokens, *rest)

    in_specs = (
        P(BOTH, None),
        P("dp", None),
        P("dp", None),
        P("expert", None, "dp"),
        P("expert", None, "dp"),
        P("expert", "dp", None),
        P(BOTH, None),
        P(BOTH, None),
    )
    out_specs = (P(BOTH, None), P(BOTH, None), P(BOTH, None))
    return jax.shard_map(
        on_device, mesh=mesh, in_specs=in_specs, out_specs=out_specs, check_vma=False
    )
```

```python
import functools

import jax
import jax.numpy as jnp
from jax import lax
from jax.experimental import pallas as pl
from jax.experimental.pallas import tpu as pltpu
from jax.sharding import PartitionSpec as P

epsilon = 1e-05
BOTH = ("dp", "expert")
ROOM = 1 << 21
SHARES = (4, 5, 7, 8)
POOL_ROWS = 18432
VMEM_LIMIT = 55000000
PAIR = 2
F32 = jnp.float32
BF16 = jnp.bfloat16


def rms_normed(values):
    return values * lax.rsqrt(jnp.mean(values * values, axis=-1, keepdims=True) + epsilon)


def pair_weights(logits, chosen):
    picked = jnp.take_along_axis(logits, chosen, axis=1)
    first = jax.nn.sigmoid(picked[:, 0] - picked[:, 1])
    return jnp.stack([first, 1.0 - first], axis=1)


def layer_kernel(
    depth, sizes,
    tokens_hbm, now_hbm, next_hbm, gate_hbm, up_hbm, down_hbm, ids_hbm, next_ids_hbm,
    out_ref, logits_ref, weights_ref,
    tok, now_own, next_own, ids_ref, next_ids_ref, now_low, now_all, next_all, xbuf, pool, acc, hidden,
    part, rd, ra, rb, rz, table,
    local_sem, in_sem, down_sem, small_send, small_recv,
    ag_send, ag_z, ag_pair, ag_core, rs_send, rs_core, rs_first, rs_second, rs_z,
    own_first, own_second,
):
    experts, width, units = gate_hbm.shape
    blocks, per, _ = xbuf.shape
    chunks = len(sizes)
    starts = [sum(sizes[:c]) for c in range(chunks)]
    halves, _, _, _, wide = part.shape
    count = now_own.shape[0]
    mine = now_own.shape[1]
    rows = blocks * per
    groups = width // wide
    space = pool.shape[0]
    deep = experts * units
    Z = depth

    loads, place = [], 0
    for c in range(chunks):
        for e in range(experts):
            loads.append((place, sizes[c]))
            place += sizes[c]
    pieces = len(loads)
    down_base = place % space
    for n in range(groups):
        loads.append((place, deep))
        place += deep
    after = []
    for i, (start, size) in enumerate(loads):
        assert start // space == (start + size - 1) // space
        low, high = start - space, start + size - space
        held = [k for k in range(i) if loads[k][0] < high and sum(loads[k]) > low]
        after.append(max(held, default=-1))
    early = sum(1 for k in after[:pieces] if k < 0)
    assert max(after) < pieces

    d = lax.axis_index("dp")
    x = lax.axis_index("expert")
    core = lax.rem(d, 2)
    y = lax.rem(d // 2, 2)
    z = d // 4

    def peer(dk, dx, dy, dz):
        there = (lax.rem(z + dz, Z) * 2 + lax.rem(y + dy, 2)) * 2 + lax.rem(core + dk, 2)
        return {"dp": there, "expert": lax.rem(x + dx, 2)}

    def remote(src, dst, send, recv, to):
        return pltpu.make_async_remote_copy(
            src_ref=src, dst_ref=dst, send_sem=send, recv_sem=recv,
            device_id=to, device_id_type=pl.DeviceIdType.MESH,
        )

    near = peer(1, 0, 0, 0)
    far_first = sorted(range(1, Z), key=lambda dz: abs(2 * dz - Z))

    def in_copies(c, e):
        at = lax.rem(loads[c * experts][0] + e * sizes[c], space)
        at = pl.ds(pl.multiple_of(at, 256), sizes[c])
        rows_at = pl.ds(starts[c], sizes[c])
        return [
            pltpu.make_async_copy(
                w.at[e, rows_at, :], pool.at[at, pl.ds(g * units, units)],
                in_sem.at[c * experts + e, g],
            )
            for g, w in enumerate((gate_hbm, up_hbm))
        ]

    def down_copies(n):
        at = pl.ds(pl.multiple_of(n * wide, 128), wide)
        base = lax.rem(down_base + n * deep, space)
        return [
            pltpu.make_async_copy(
                down_hbm.at[e, :, at],
                pool.at[pl.ds(pl.multiple_of(base + e * units, 512), units), :],
                down_sem.at[n, e],
            )
            for e in range(experts)
        ]

    small = [
        pltpu.make_async_copy(source, target, local_sem.at[i])
        for i, (source, target) in enumerate((
            (tokens_hbm, tok), (now_hbm, now_own), (next_hbm, next_own),
            (ids_hbm, ids_ref), (next_ids_hbm, next_ids_ref),
        ))
    ]
    small[0].start()
    barrier = pltpu.get_barrier_semaphore()
    others = [
        (dk, dx, dy, dz)
        for dk in range(2) for dx in range(2) for dy in range(2) for dz in range(Z)
    ][1:]
    for to in others:
        pl.semaphore_signal(
            barrier, inc=1, device_id=peer(*to), device_id_type=pl.DeviceIdType.MESH
        )

    for copy in small[1:]:
        copy.start()
    for p in range(experts):
        for copy in in_copies(0, p):
            copy.start()

    small[0].wait()
    resid = tok[...].astype(F32)
    scale = lax.rsqrt(jnp.mean(resid * resid, axis=1, keepdims=True) + epsilon)
    rounded = (resid * scale).astype(BF16)
    for c in range(chunks):
        xbuf[0, :, starts[c]:starts[c] + sizes[c]] = rounded[:, starts[c]:starts[c] + sizes[c]]
    own_at = pl.ds(pl.multiple_of(d * mine, 128), mine)
    pl.semaphore_wait(barrier, len(others))

    same_side = [to for to in others if to[1] == 0]

    def send_router(own, everyone, i):
        for to in same_side:
            remote(own, everyone.at[:, own_at], small_send.at[i], small_recv.at[i], peer(*to)).start()

    def router_bytes(everyone, i):
        span = everyone.at[:, pl.ds(0, mine * len(same_side))]
        return remote(span, span, small_send.at[i], small_recv.at[i], near)

    def choose(values, ids):
        eye = lax.broadcasted_iota(jnp.int32, (per, per), 0) == lax.broadcasted_iota(
            jnp.int32, (per, per), 1
        )
        names = [
            jnp.sum(jnp.where(eye, ids[i:i + 1, :].astype(F32), 0.0), axis=1, keepdims=True)
            for i in range(2)
        ]
        picked = [
            sum(jnp.where(name == float(e), values[e], 0.0) for e in range(count)) for name in names
        ]
        first = 1.0 / (1.0 + jnp.exp(picked[1] - picked[0]))
        return names, first

    def route(c):
        now_all[:, own_at] = now_low[...]
        router_bytes(now_all, 0).wait_recv()
        whole = now_all[...].astype(F32)
        held = tok[...].astype(F32)
        values = [
            jnp.sum(held * whole[e:e + 1, :], axis=1, keepdims=True) * scale for e in range(count)
        ]
        names, first = choose(values, ids_ref[...])
        lane = lax.broadcasted_iota(jnp.int32, (per, 128), 1).astype(F32)
        table[0] = jnp.where(lane == names[0], first, 0.0) + jnp.where(
            lane == names[1], 1.0 - first, 0.0
        )
        for dk, dx, dy, dz in others:
            slot = ((dk * 2 + dx) * 2 + dy) * Z + (Z - dz) % Z
            remote(
                table.at[0], table.at[slot], small_send.at[1], small_recv.at[1], peer(dk, dx, dy, dz)
            ).start()

    def table_bytes():
        span = table.at[pl.ds(1, len(others))]
        return remote(span, span, small_send.at[1], small_recv.at[1], near)

    own_piece, rest_piece = (0, 1), (1, Z - 1)
    Y_LINE, X_LINE, FAR_LINE, CORE = Z, 2 * Z, 3 * Z, 4 * Z
    y_peer, x_peer = peer(0, 0, 1, 0), peer(0, 1, 0, 0)

    def lines(c):
        return ((Y_LINE, y_peer, X_LINE, x_peer) if c % 2 == 0 else (X_LINE, x_peer, Y_LINE, y_peer))

    def piece(c, start, size):
        return xbuf.at[pl.ds(start, size), :, pl.ds(starts[c], sizes[c])]

    def hop(c, which, part_index, source, target, to):
        start, size = (own_piece, rest_piece)[part_index]
        return remote(
            piece(c, source + start, size), piece(c, target + start, size),
            ag_send.at[c], ag_pair.at[c, which, part_index], to,
        )

    def across(c, i):
        return remote(
            piece(c, i * Z, Z), piece(c, CORE + i * Z, Z),
            ag_send.at[c], ag_core.at[c, i], near,
        )

    def gather_first(c):
        a, a_peer, b, b_peer = lines(c)
        hop(c, 0, 0, 0, a, a_peer).start()
        hop(c, 1, 0, 0, b, b_peer).start()
        for dz in far_first:
            remote(
                piece(c, 0, 1), piece(c, Z - dz, 1), ag_send.at[c], ag_z.at[c], peer(0, 0, 0, dz)
            ).start()

    def gather_own(c):
        a, a_peer, b, b_peer = lines(c)
        hop(c, 0, 0, 0, a, a_peer).wait_recv()
        hop(c, 2, 0, a, FAR_LINE, b_peer).start()

    def gather_line(c):
        span = piece(c, 1, Z - 1)
        remote(span, span, ag_send.at[c], ag_z.at[c], near).wait_recv()
        a, a_peer, b, b_peer = lines(c)
        hop(c, 0, 1, 0, a, a_peer).start()
        hop(c, 1, 1, 0, b, b_peer).start()
        across(c, 0).start()

    def gather_far(c):
        a, a_peer, b, b_peer = lines(c)
        hop(c, 0, 1, 0, a, a_peer).wait_recv()
        hop(c, 2, 1, a, FAR_LINE, b_peer).start()
        across(c, a // Z).start()

    def gather_second(c):
        a, a_peer, b, b_peer = lines(c)
        for i in range(2):
            hop(c, 1, i, 0, b, b_peer).wait_recv()
        across(c, b // Z).start()

    def gather_last(c):
        a, a_peer, b, b_peer = lines(c)
        for i in range(2):
            hop(c, 2, i, a, FAR_LINE, b_peer).wait_recv()
        across(c, 3).start()

    def gather_done(c):
        for i in range(4):
            across(c, i).wait_recv()

    for c in range(chunks):
        gather_first(c)
    for copy in small[1:]:
        copy.wait()
    now_low[...] = now_own[...].astype(BF16)
    send_router(now_low, now_all, 0)
    for p in range(experts, early):
        for copy in in_copies(p // experts, p % experts):
            copy.start()

    hooks = {
        -1: [
            (gather_own, 0), (gather_own, 1), (gather_line, 0), (gather_own, 2), (gather_own, 3),
            (gather_line, 1), (gather_far, 0), (gather_second, 0), (gather_far, 1),
            (gather_second, 1), (gather_line, 2), (gather_last, 0), (gather_line, 3),
        ],
        0: [(gather_done, 0)],
        2: [(gather_last, 1)],
        4: [(gather_far, 2), (gather_second, 2), (gather_done, 1)],
        6: [(route, 0), (gather_far, 3)],
        8: [(gather_last, 2), (gather_second, 3), (gather_done, 2)],
        10: [(gather_last, 3)],
        12: [(gather_done, 3)],
    }
    for action, c in hooks.pop(-1):
        action(c)

    freed = {}
    for i in range(early, len(loads)):
        freed.setdefault(max(after[i], 0), []).append(i)

    lane = lax.broadcasted_iota(jnp.int32, (rows, 128), 1)

    def ahead(c, i, carry):
        for step in range(c * experts, (c + 1) * experts, PAIR):
            if step in hooks:
                @pl.when(i * PAIR == step - c * experts)
                def _(actions=hooks[step]):
                    for action, at in actions:
                        action(at)

        for k in range(PAIR):
            for copy in in_copies(c, i * PAIR + k):
                copy.wait()
        for k in range(PAIR):
            e = i * PAIR + k
            at = lax.rem(loads[c * experts][0] + e * sizes[c], space)
            at = pl.ds(pl.multiple_of(at, 256), sizes[c])
            value = jnp.dot(
                xbuf[:, :, starts[c]:starts[c] + sizes[c]].reshape(rows, sizes[c]), pool[at, :],
                preferred_element_type=F32,
            )
            if c == 0:
                acc[e] = value
            elif c < chunks - 1:
                acc[e] += value
            else:
                value = value + acc[e]
                gate, upward = value[:, :units], value[:, units:]
                share = jnp.sum(
                    jnp.where(lane == x * experts + e, table[...].reshape(rows, 128), 0.0),
                    axis=1, keepdims=True,
                )
                value = gate / (1.0 + jnp.exp(-gate)) * upward * share
                hidden[:, pl.ds(pl.multiple_of(e * units, 128), units)] = value.astype(BF16)

        for first in range(c * experts, (c + 1) * experts, PAIR):
            steps = range(first, first + PAIR)
            if any(step in freed for step in steps):
                @pl.when(i * PAIR == first - c * experts)
                def _(steps=steps):
                    for step in steps:
                        for load in freed.get(step, []):
                            if load < pieces:
                                copies = in_copies(load // experts, load % experts)
                            else:
                                copies = down_copies(load - pieces)
                            for copy in copies:
                                copy.start()

        return carry

    for c in range(chunks):
        if c == 1:
            next_all[:, own_at] = next_own[...]
        if c == chunks - 1:
            send_router(next_own, next_all, 2)
            table_bytes().wait_recv()
        lax.fori_loop(0, experts // PAIR, functools.partial(ahead, c), 0)

    REST = pl.ds(1, Z - 1)

    def scatter_core(c):
        h, p = c // 2, c % 2
        return remote(
            part.at[h, p, pl.ds(CORE, CORE)], rd.at[h, p], rs_send.at[0], rs_core.at[h, p], near
        )

    def reverse(p):
        return ((X_LINE, x_peer, Y_LINE, y_peer) if p == 0 else (Y_LINE, y_peer, X_LINE, x_peer))

    def scatter_first(c, i):
        h, p = c // 2, c % 2
        a, a_peer, b, b_peer = reverse(p)
        source = (a, FAR_LINE)[i]
        return remote(
            part.at[h, p, pl.ds(source + 1, Z - 1)], ra.at[h, p, i, REST],
            rs_send.at[0], rs_first.at[h, p, i], a_peer,
        )

    def scatter_second(c):
        h, p = c // 2, c % 2
        a, a_peer, b, b_peer = reverse(p)
        return remote(
            part.at[h, p, pl.ds(b + 1, Z - 1)], rb.at[h, p, REST],
            rs_send.at[0], rs_second.at[h, p], b_peer,
        )

    def layer_first(p, i):
        a, a_peer, b, b_peer = reverse(p)
        source = (a, FAR_LINE)[i]
        return remote(
            part.at[:, p, source], ra.at[:, p, i, 0], rs_send.at[0], own_first.at[p, i], a_peer
        )

    def layer_second(p):
        a, a_peer, b, b_peer = reverse(p)
        return remote(
            part.at[:, p, b], rb.at[:, p, 0], rs_send.at[0], own_second.at[p], b_peer
        )

    def add_core(c):
        h, p = c // 2, c % 2
        scatter_core(c).wait_recv()
        a, a_peer, b, b_peer = reverse(p)

        def add(at):
            span = pl.ds(at, Z)
            part[h, p, span] = (
                part[h, p, span].astype(F32) + rd[h, p, span].astype(F32)
            ).astype(BF16)

        add(FAR_LINE)
        scatter_first(c, 1).start()
        add(a)
        scatter_first(c, 0).start()
        add(b)
        add(0)

    def add_first(c):
        h, p = c // 2, c % 2
        a, a_peer, b, b_peer = reverse(p)
        scatter_first(c, 1).wait_recv()
        span = pl.ds(b + 1, Z - 1)
        part[h, p, span] = (
            part[h, p, span].astype(F32) + ra[h, p, 1, REST].astype(F32)
        ).astype(BF16)
        scatter_second(c).start()

    def add_second(c):
        h, p = c // 2, c % 2
        scatter_first(c, 0).wait_recv()
        scatter_second(c).wait_recv()
        part[h, p, REST] = (
            part[h, p, REST].astype(F32)
            + ra[h, p, 0, REST].astype(F32) + rb[h, p, REST].astype(F32)
        ).astype(BF16)
        for dz in far_first:
            remote(
                part.at[h, p, dz], rz.at[h, p, Z - 1 - dz],
                rs_send.at[0], rs_z.at[h, p], peer(0, 0, 0, dz),
            ).start()

    def layer_send(p):
        for i in (1, 0):
            layer_first(p, i).start()

    def layer_add(p):
        a, a_peer, b, b_peer = reverse(p)
        layer_first(p, 1).wait_recv()
        part[:, p, b] = (part[:, p, b].astype(F32) + ra[:, p, 1, 0].astype(F32)).astype(BF16)
        layer_second(p).start()

    def layer_wait(p):
        layer_first(p, 0).wait_recv()
        layer_second(p).wait_recv()

    ready = {groups - 3: (0,), groups - 2: (1,), groups - 1: (2,)}

    def down(n, carry):
        for copy in down_copies(n):
            copy.wait()
        at = pl.multiple_of(lax.rem(down_base + n * deep, space), 512)
        total = jnp.dot(
            hidden[...], pool[pl.ds(at, experts * units), :], preferred_element_type=F32
        )
        part[n // 2, lax.rem(n, 2)] = total.astype(BF16).reshape(blocks, per, wide)
        for k in range(groups):
            @pl.when(n == k)
            def _(k=k):
                scatter_core(k).start()
                if k:
                    add_core(k - 1)
                for c in ready.get(k, ()):
                    add_first(c)
                if k == groups - 1:
                    add_second(0)

        return carry

    lax.fori_loop(0, groups, down, 0)

    held = {"square": jnp.zeros((per, 1), F32), "values": [jnp.zeros((per, 1), F32)] * count}

    def finish(c):
        h, p = c // 2, c % 2
        span = rz.at[h, p]
        remote(span, span, rs_send.at[0], rs_z.at[h, p], near).wait_recv()
        at = slice(c * wide, (c + 1) * wide)
        mixture = part[h, p, 0].astype(F32) + ra[h, p, 0, 0].astype(F32) + rb[h, p, 0].astype(F32)
        for i in range(Z - 1):
            mixture = mixture + rz[h, p, i].astype(F32)
        summed = tok[:, at].astype(F32) + mixture
        out_ref[:, at] = summed.astype(BF16)
        held["square"] = held["square"] + jnp.sum(summed * summed, axis=1, keepdims=True)
        held["values"] = [
            held["values"][e]
            + jnp.sum(summed * next_all[e:e + 1, at], axis=1, keepdims=True)
            for e in range(count)
        ]

    def next_wait(i):
        router_bytes(next_all, i).wait_recv()

    last = groups - 1
    order = [(add_core, last)]
    for c in range(3, groups):
        order += [(add_first, c), (add_second, c - 2)]
    order[-1:-1] = [(layer_send, 0), (layer_send, 1)]
    order += [(add_second, last - 1), (add_second, last), (layer_add, 0), (layer_add, 1)]
    order += [(next_wait, 2), (layer_wait, 0)] + [(finish, c) for c in range(0, last - 1, 2)]
    order += [(layer_wait, 1)] + [(finish, c) for c in range(1, last, 2)]
    order += [(finish, last - 1), (finish, last)]
    for action, c in order:
        action(c)

    final = lax.rsqrt(held["square"] / float(width) + epsilon)
    values = [value * final for value in held["values"]]
    place = lax.broadcasted_iota(jnp.int32, (per, count), 1)
    logits_ref[...] = sum(jnp.where(place == e, values[e], 0.0) for e in range(count))
    names, first = choose(values, next_ids_ref[...])
    eye = lax.broadcasted_iota(jnp.int32, (per, per), 0) == lax.broadcasted_iota(
        jnp.int32, (per, per), 1
    )
    for i, value in enumerate((first, 1.0 - first)):
        weights_ref[i:i + 1, :] = jnp.sum(jnp.where(eye, value, 0.0), axis=0, keepdims=True)

    router_bytes(now_all, 0).wait_send()
    router_bytes(next_all, 2).wait_send()
    table_bytes().wait_send()
    for c in range(chunks):
        span = piece(c, 1, blocks - 1)
        remote(span, span, ag_send.at[c], ag_z.at[c], near).wait_send()
    span = part.at[:, :, pl.ds(1, blocks - 1)]
    remote(span, span, rs_send.at[0], rs_z.at[0, 0], near).wait_send()


def fused_layer(
    dp, tokens, router_now, router_next, w_gate, w_up, w_down, expert_ids, next_ids
):
    experts, width, units = w_gate.shape
    per = tokens.shape[0]
    mine, count = router_now.shape
    depth = dp // 4
    blocks = dp * 2
    rows = blocks * per
    sizes = tuple(width // sum(SHARES) * share for share in SHARES)
    chunks = len(sizes)
    wide = 2 * units
    pieces = chunks * experts
    groups = width // wide
    halves = groups // 2
    vmem = pl.BlockSpec(memory_space=pltpu.VMEM)
    hbm = pl.BlockSpec(memory_space=pltpu.HBM)
    dma = pltpu.SemaphoreType.DMA
    stay = functools.partial(pltpu.with_memory_space_constraint, memory_space=pltpu.HBM)
    layer_out, next_logits, next_weights = pl.pallas_call(
        functools.partial(layer_kernel, depth, sizes),
        out_shape=[
            jax.ShapeDtypeStruct((per, width), BF16),
            jax.ShapeDtypeStruct((per, count), F32),
            jax.ShapeDtypeStruct((2, per), F32),
        ],
        in_specs=[hbm] * 8,
        out_specs=[vmem] * 3,
        scratch_shapes=[
            pltpu.VMEM((per, width), BF16),
            pltpu.VMEM((count, mine), F32),
            pltpu.VMEM((count, mine), F32),
            pltpu.VMEM((2, per), jnp.int32),
            pltpu.VMEM((2, per), jnp.int32),
            pltpu.VMEM((count, mine), BF16),
            pltpu.VMEM((count, width), BF16),
            pltpu.VMEM((count, width), F32),
            pltpu.VMEM((blocks, per, width), BF16),
            pltpu.VMEM((POOL_ROWS, wide), BF16),
            pltpu.VMEM((experts, rows, wide), F32),
            pltpu.VMEM((rows, experts * units), BF16),
            pltpu.VMEM((halves, 2, blocks, per, wide), BF16),
            pltpu.VMEM((halves, 2, blocks // 2, per, wide), BF16),
            pltpu.VMEM((halves, 2, 2, depth, per, wide), BF16),
            pltpu.VMEM((halves, 2, depth, per, wide), BF16),
            pltpu.VMEM((halves, 2, depth - 1, per, wide), BF16),
            pltpu.VMEM((blocks, per, 128), F32),
            dma((5,)),
            dma((pieces, 2)),
            dma((groups, experts)),
            dma((3,)),
            dma((3,)),
            dma((chunks,)),
            dma((chunks,)),
            dma((chunks, 3, 2)),
            dma((chunks, 4)),
            dma((1,)),
            dma((halves, 2)),
            dma((halves, 2, 2)),
            dma((halves, 2)),
            dma((halves, 2)),
            dma((2, 2)),
            dma((2,)),
        ],
        compiler_params=pltpu.CompilerParams(
            vmem_limit_bytes=VMEM_LIMIT, collective_id=0, has_side_effects=True
        ),
    )(
        *[stay(value) for value in (tokens, router_now.T, router_next.T)],
        w_gate, w_up, w_down, stay(expert_ids.T), stay(next_ids.T),
    )
    return layer_out, next_logits, next_weights.T


def gathered_layer(tokens, router_now, router_next, w_gate, w_up, w_down, expert_ids, next_ids):
    experts, width, units = w_gate.shape
    count = router_now.shape[1]
    resid = tokens.astype(F32)
    normed = rms_normed(resid)
    pair = lax.all_gather(normed.astype(BF16), "expert", axis=0, tiled=True)
    everyone = lax.all_gather(pair, "dp", axis=0, tiled=True)
    rows = everyone.shape[0]
    routers = jnp.concatenate([router_now.T, router_next.T], axis=0)
    routers = lax.all_gather(routers, "dp", axis=1, tiled=True)
    whole_now, whole_next = routers[:count], routers[count:]
    exact = functools.partial(
        lax.dot_general,
        dimension_numbers=(((1,), (1,)), ((), ())),
        precision=lax.Precision.HIGHEST,
        preferred_element_type=F32,
    )
    logits = exact(normed, whole_now)
    weights = pair_weights(logits, expert_ids)
    named = expert_ids[:, :, None] == jnp.arange(count, dtype=jnp.int32)[None, None, :]
    table = jnp.sum(jnp.where(named, weights[:, :, None], 0.0), axis=1)
    table = lax.all_gather(table, BOTH, axis=0, tiled=True)
    share = lax.dynamic_slice_in_dim(table, lax.axis_index("expert") * experts, experts, axis=1)
    share = share.T[:, :, None]
    total = jnp.zeros((rows, width), F32)
    for e in range(experts):
        gate = jnp.dot(everyone, w_gate[e], preferred_element_type=F32)
        upward = jnp.dot(everyone, w_up[e], preferred_element_type=F32)
        value = gate / (1.0 + jnp.exp(-gate)) * upward * share[e]
        total = total + jnp.dot(value.astype(BF16), w_down[e], preferred_element_type=F32)
    mixture = lax.psum_scatter(total.astype(BF16), "dp", scatter_dimension=0, tiled=True)
    mixture = lax.psum_scatter(mixture, "expert", scatter_dimension=0, tiled=True)
    summed = resid + mixture.astype(F32)
    next_logits = exact(rms_normed(summed), whole_next)
    return (summed.astype(BF16), next_logits, pair_weights(next_logits, next_ids))


def solution(mesh):
    dp, sides = mesh.shape["dp"], mesh.shape["expert"]

    def on_device(tokens, *rest):
        rows, width = tokens.shape[0] * dp * sides, tokens.shape[1]
        if sides == 2 and dp % 4 == 0 and rows * width <= ROOM:
            return fused_layer(dp, tokens, *rest)
        return gathered_layer(tokens, *rest)

    in_specs = (
        P(BOTH, None),
        P("dp", None),
        P("dp", None),
        P("expert", None, "dp"),
        P("expert", None, "dp"),
        P("expert", "dp", None),
        P(BOTH, None),
        P(BOTH, None),
    )
    out_specs = (P(BOTH, None), P(BOTH, None), P(BOTH, None))
    return jax.shard_map(
        on_device, mesh=mesh, in_specs=in_specs, out_specs=out_specs, check_vma=False
    )
```
